256 devices in a mesh: patch: 128 (over y, z, x), pix: 2 (over core).
Axes of the slice: x: 4, y: 4, z: 8, core: 2. Of those that a mesh axis runs over, the one named last changes fastest.
Arguments:
- pixel_pos: float32 [2, 24576], P(None, ('patch', 'pix')), may hold values from -4 to 4
- pixel_view: float32 [3, 24576], P(None, ('patch', 'pix')), may hold values from -1 to 1
- observed: float32 [24576], P(('patch', 'pix')), may hold values from -6 to 6
- noise_scale: float32 [24576], P(('patch', 'pix')), may hold values from 0.5 to 2
- valid_mask: int32 [24576], P(('patch', 'pix')), may hold values 0 or 1
- patch_pos: float32 [2, 6144], P(None, 'patch'), may hold values from -4 to 4
- patch_depth: float32 [6144], P('patch'), may hold values from 0.3 to 1.5
- segment_ids: int32 [6144], P('patch'), may hold values from 0 to 15, never falling along the last dimension, each value on 1 to 1536 neighbouring positions
- seg_strike: float32 [16], replicated, may hold values from -3.140625 to 3.140625
- seg_dip: float32 [16], replicated, may hold values from 0.35 to 1.4
- slip_models: bfloat16 [6144, 3, 128], P('patch'), may hold values from -0.8984375 to 0.8984375
Outputs:
- residual: float32 [24576, 128], P(('patch', 'pix'))
- misfit: float32 [128], replicated
The draws below stay inside these ranges and needn't reach their ends.
Inputs may be any that keep to these rules, and one draw needn't show every extreme that they name: `segment_ids`: segment ids never fall along the patches.
All inputs are finite; a program needn't handle non-finite values. No bound on the sum of `valid_mask` on one device may be relied on, other than what follows from the above.
Results may differ from the reference program's by a relative error of at most 0.0003.
Values may be sent and summed in bfloat16 or wider, within the bound.
No kernel may reach another device: no remote copies, remote signals or barrier semaphores. Data moves between devices by JAX's collectives and lax.ppermute only.
A program may use at most 64 MiB of HBM per device.

```python
import math
import jax
import jax.numpy as jnp
import numpy as np
from jax import lax

PATCH_DEV = 48
SAMPLES = 128
SEGMENTS = 16
PATCHES = 6144
PIXELS = 24576
N_PATCH = 128


def touch_ends(values, rng, least, top_value):
    spot = [jax.random.randint(jax.random.fold_in(rng, axis), (), 0, length) for axis, length in enumerate(values.shape)]
    longest = values.shape.index(max(values.shape))
    neighbour = spot[:longest] + [(spot[longest] + 1) % values.shape[longest]] + spot[longest + 1:]
    return values.at[tuple(spot)].set(least).at[tuple(neighbour)].set(top_value)


def block_scale(own_key, dims, shards, smallest, top_value):
    def one(dim, parts):
        draws = jax.random.uniform(jax.random.fold_in(jax.random.fold_in(own_key, 6), dim), (parts,), jnp.float32, smallest / len(shards), top_value / len(shards))
        return jnp.repeat(jnp.exp(draws), dims[dim] // parts).reshape((-1,) + (1,) * (len(dims) - dim - 1))

    loudness = one(*shards[0])
    for cut in shards[1:]:
        loudness = loudness * one(*cut)
    return loudness


def split_up(number_of, total, most, slope):
    portions = [(1 << 20) // math.isqrt(standing ** slope) + 1 for standing in range(2, number_of + 1)]
    surplus, counts = total - most - (number_of - 1), [1] * (number_of - 1)
    while surplus > 0:
        candidates = [i for i in range(number_of - 1) if counts[i] < most]
        mass, remaining = sum([portions[i] for i in candidates]), surplus
        for i in candidates:
            more = min(most - counts[i], max(1, remaining * portions[i] // mass), surplus)
            counts[i] = counts[i] + more
            surplus = surplus - more
    return np.array([most] + counts)


def ragged_sizes(own_key, count, total, most, skew):
    if count == 2:
        one = jax.random.randint(own_key, (), max(1, total - most), min(most, total - 1) + 1)
        return jnp.stack([one, total - one])
    tallies = jnp.asarray(split_up(count, total, most, skew), jnp.int32)
    couples = (count - 1) // 2
    source_of, receiver = tallies[1:1 + 2 * couples:2], tallies[2:2 + 2 * couples:2]
    room = jnp.minimum(source_of - 1, most - receiver)
    shifted = jax.random.randint(jax.random.fold_in(own_key, 1), (couples,), 0, 1 << 20) % (room + 1)
    tallies = tallies.at[1:1 + 2 * couples:2].set(source_of - shifted).at[2:2 + 2 * couples:2].set(receiver + shifted)
    return tallies[jax.random.permutation(jax.random.fold_in(own_key, 2), count)]


def normal_values(own_key, dims, spread, bound, shards=(), kind=jnp.bfloat16):
    array = jax.random.normal(own_key, dims, jnp.float32) * spread
    if len(shards) > 0:
        array = block_scale(own_key, dims, shards, -0.22, 0.18) * array
    return jnp.clip(array, min=-bound, max=bound).astype(kind)


def setup_inputs(seed: int = 0) -> dict:
    keys = jax.random.split(jax.random.key(seed), 12)
    pixel_pos = jnp.clip(jax.random.uniform(keys[0], (2, PIXELS), jnp.float32, -4.0, 4.0) * block_scale(keys[0], (2, PIXELS), ((1, 256),), -0.4, 0.0), -4.0, 4.0)
    pixel_view = jnp.clip(jax.random.uniform(keys[1], (3, PIXELS), jnp.float32, -1.0, 1.0) * block_scale(keys[1], (3, PIXELS), ((1, 256),), -0.4, 0.0), -1.0, 1.0)
    observed = normal_values(keys[2], (PIXELS,), 1.0, 6.0, ((0, 256),), jnp.float32)
    noise_scale = jnp.clip(jnp.exp(math.log(2.0) - 1.3862944 * jax.random.uniform(keys[3], (PIXELS,), jnp.float32) ** block_scale(keys[3], (PIXELS,), ((0, 256),), -0.2, 0.2)), 0.5, 2.0)
    valid_mask = touch_ends((jax.random.randint(keys[4], (PIXELS,), 0, 8) < 7).astype(jnp.int32), jax.random.fold_in(keys[4], 1), 0, 1)
    patch_pos = jnp.clip(jax.random.uniform(keys[5], (2, PATCHES), jnp.float32, -4.0, 4.0) * block_scale(keys[5], (2, PATCHES), ((1, 128),), -0.4, 0.0), -4.0, 4.0)
    patch_depth = jnp.clip(0.3 + 1.2 * jax.random.uniform(keys[6], (PATCHES,), jnp.float32) ** block_scale(keys[6], (PATCHES,), ((0, 128),), -0.2, 0.2), 0.3, 1.5)
    segment_ids = jnp.searchsorted(jnp.cumsum(ragged_sizes(keys[7], SEGMENTS, PATCHES, PATCH_DEV * N_PATCH // 4, 1)), jnp.arange(PATCHES), side="right").astype(jnp.int32)
    seg_strike = jnp.clip(jax.random.uniform(keys[8], (SEGMENTS,), jnp.float32, -3.140625, 3.140625), -3.140625, 3.140625)
    seg_dip = jnp.clip(jax.random.uniform(keys[9], (SEGMENTS,), jnp.float32, 0.35, 1.4), 0.35, 1.4)
    slip_models = normal_values(keys[10], (PATCHES, 3, SAMPLES), 0.15, 0.8984375, ((0, 128),))
    return {"pixel_pos": pixel_pos, "pixel_view": pixel_view, "observed": observed, "noise_scale": noise_scale, "valid_mask": valid_mask, "patch_pos": patch_pos, "patch_depth": patch_depth, "segment_ids": segment_ids, "seg_strike": seg_strike, "seg_dip": seg_dip, "slip_models": slip_models}


two_pi = 2.0 * math.pi
mu_ratio = 0.5

def point_green(pixel_pos, pixel_view, frame_rows):
    src_east = frame_rows[0][:, None]
    src_north = frame_rows[1][:, None]
    src_depth = frame_rows[2][:, None]
    sin_strike = frame_rows[3][:, None]
    cos_strike = frame_rows[4][:, None]
    sin_dip = frame_rows[5][:, None]
    cos_dip = frame_rows[6][:, None]
    east_gap = pixel_pos[0][None, :] - src_east
    north_gap = pixel_pos[1][None, :] - src_north
    along_x = east_gap * sin_strike + north_gap * cos_strike
    across = north_gap * sin_strike - east_gap * cos_strike
    depth_term = across * cos_dip + src_depth * sin_dip
    plane_term = across * sin_dip - src_depth * cos_dip
    radius = jnp.sqrt(along_x * along_x + across * across + src_depth * src_depth)
    over_r = 1.0 / radius
    over_r3 = over_r * over_r * over_r
    over_r5 = over_r3 * over_r * over_r
    over_rd = 1.0 / (radius + src_depth)
    base_term = over_r * over_rd * over_rd
    cubic_term = (3.0 * radius + src_depth) * over_r3 * over_rd * over_rd * over_rd
    square_term = (2.0 * radius + src_depth) * over_r3 * over_rd * over_rd
    term_one = mu_ratio * across * (base_term - along_x * along_x * cubic_term)
    term_two = mu_ratio * along_x * (base_term - across * across * cubic_term)
    term_three = mu_ratio * along_x * over_r3 - term_two
    term_four = -mu_ratio * along_x * across * square_term
    term_five = mu_ratio * (over_r * over_rd - along_x * along_x * square_term)
    scaled_q = 3.0 * plane_term * over_r5
    dip_mixed = sin_dip * cos_dip
    dip_square = sin_dip * sin_dip
    strike_x = -(scaled_q * along_x * along_x + term_one * sin_dip)
    strike_y = -(scaled_q * along_x * across + term_two * sin_dip)
    strike_z = -(scaled_q * along_x * src_depth + term_four * sin_dip)
    dip_x = -(scaled_q * along_x * depth_term - term_three * dip_mixed)
    dip_y = -(scaled_q * across * depth_term - term_one * dip_mixed)
    dip_z = -(scaled_q * src_depth * depth_term - term_five * dip_mixed)
    open_x = scaled_q * along_x * plane_term - term_three * dip_square
    open_y = scaled_q * across * plane_term - term_one * dip_square
    open_z = scaled_q * src_depth * plane_term - term_five * dip_square

    def project(comp_x, comp_y, comp_z):
        east_move = comp_x * sin_strike - comp_y * cos_strike
        north_move = comp_x * cos_strike + comp_y * sin_strike
        return (pixel_view[0][None, :] * east_move + pixel_view[1][None, :] * north_move + pixel_view[2][None, :] * comp_z) / two_pi
    return jnp.stack([project(strike_x, strike_y, strike_z), project(dip_x, dip_y, dip_z), project(open_x, open_y, open_z)], axis=1)

def reference(pixel_pos, pixel_view, observed, noise_scale, valid_mask, patch_pos, patch_depth, segment_ids, seg_strike, seg_dip, slip_models):
    strike = jnp.take(seg_strike, segment_ids)
    dip_angle = jnp.take(seg_dip, segment_ids)
    frames = jnp.stack([patch_pos[0], patch_pos[1], patch_depth, jnp.sin(strike), jnp.cos(strike), jnp.sin(dip_angle), jnp.cos(dip_angle)], axis=0)
    patch_count = patch_depth.shape[0]
    block_size = math.gcd(patch_count, 64)
    block_count = patch_count // block_size
    samples = slip_models.shape[2]
    framed = frames.reshape(7, block_count, block_size).transpose(1, 0, 2)
    slip_blocks = slip_models.reshape(block_count, block_size * 3, samples)

    def add_block(running, block_items):
        frame_rows, block_slip = block_items
        green_tile = point_green(pixel_pos, pixel_view, frame_rows).astype(jnp.bfloat16)
        green_tile = lax.optimization_barrier(green_tile).reshape(block_size * 3, PIXELS)
        part_sum = lax.dot_general(green_tile.astype(jnp.float32), block_slip.astype(jnp.float32), (((0,), (0,)), ((), ())), precision=lax.Precision.HIGHEST)
        return (running + part_sum, None)
    predicted, _ = lax.scan(add_block, jnp.zeros((PIXELS, samples), jnp.float32), (framed, slip_blocks))
    residual = valid_mask.astype(jnp.float32)[:, None] * (predicted - observed[:, None]) / noise_scale[:, None]
    misfit = lax.optimization_barrier(jnp.sum(residual * residual, axis=0)) / PIXELS
    return (residual, misfit)
```

```python
import functools
import math

import jax
import jax.numpy as jnp
from jax import lax
from jax.experimental import pallas as pl
from jax.experimental.pallas import tpu as pltpu
from jax.sharding import Mesh
from jax.sharding import PartitionSpec as P

PATCH = ("y", "z", "x")
PATCH_PIX = ("y", "z", "x", "pix")

LANES = 128
SUB = 8
GROUPS = 3
PIECE = SUB * GROUPS
SLIP_ROWS = 3 * PIECE
ROWS = SLIP_ROWS + SUB
FRAME_STRIDE = 40
UNIT = LANES // SUB
VIEW_SCALE = 3.0 / (2.0 * math.pi)


def xor_pairs(count, mask):
    return [(i, i ^ mask) for i in range(count)]


def mirror_pairs(count):
    return [(i, count - 1 - i) for i in range(count)]


def rounded(value):
    return value.astype(jnp.bfloat16).astype(jnp.float32)


def pack_kernel(core_ref, strike_ref, dip_ref, pos_ref, depth_ref, ids_ref, slip_ref, out_ref, turned_ref):
    ids = ids_ref[...]
    strike = jnp.zeros(ids.shape, jnp.float32)
    dip = jnp.zeros(ids.shape, jnp.float32)
    for segment in range(strike_ref.shape[0]):
        same = ids == segment
        strike = jnp.where(same, strike_ref[segment], strike)
        dip = jnp.where(same, dip_ref[segment], dip)
    pos = pos_ref[...]
    angles = jnp.concatenate([strike, dip], axis=0)
    sines = jnp.sin(angles)
    cosines = jnp.cos(angles)
    rows = jnp.concatenate(
        [pos, depth_ref[...], sines[0:1], cosines[0:1], sines[1:2], cosines[1:2], jnp.zeros(ids.shape, jnp.float32)],
        axis=0,
    )
    high = rounded(rows)
    rest = rows - high
    middle = rounded(rest)
    low = rounded(rest - middle)
    count = rows.shape[1]
    pieces = jnp.concatenate([high, middle, low], axis=0)
    pieces = jnp.concatenate([pieces, jnp.zeros((24, LANES - count), jnp.float32)], axis=1)
    pieces = jnp.concatenate([pieces, jnp.zeros((LANES - 24, LANES), jnp.float32)], axis=0)
    turned_ref[...] = jnp.transpose(pieces)
    first = core_ref[0] * PIECE
    tile = jnp.zeros((SUB, LANES), jnp.float32)
    for group in range(GROUPS):
        start = pl.multiple_of(first + SUB * group, SUB)
        part = turned_ref[pl.ds(start, SUB), :]
        tile = tile + (part if group == 0 else pltpu.roll(part, FRAME_STRIDE * group, 1))
        for k in range(3):
            row = (k * GROUPS + group) * SUB
            out_ref[row : row + SUB, :] = slip_ref[k, pl.ds(start, SUB), :]
    out_ref[SLIP_ROWS:ROWS, :] = tile.astype(jnp.bfloat16)


def pack(core, seg_strike, seg_dip, patch_pos, patch_depth, segment_ids, slip):
    smem = pl.BlockSpec(memory_space=pltpu.SMEM)
    vmem = pl.BlockSpec(memory_space=pltpu.VMEM)
    return pl.pallas_call(
        pack_kernel,
        out_shape=jax.ShapeDtypeStruct((ROWS, LANES), jnp.bfloat16),
        in_specs=[smem, smem, smem, vmem, vmem, vmem, vmem],
        out_specs=vmem,
        scratch_shapes=[pltpu.VMEM((LANES, LANES), jnp.float32)],
        name="pack",
    )(core, seg_strike, seg_dip, patch_pos, patch_depth[None, :], segment_ids[None, :], jnp.transpose(slip, (1, 0, 2)))


def unit_kernel(sites_ref, unit_ref, acc_ref, out_ref, pix_ref, green_ref):
    blocks, _, width = sites_ref.shape
    pixels = blocks * width
    for block in range(blocks):
        site = jnp.concatenate([sites_ref[block], jnp.zeros((SUB, LANES - width), jnp.float32)], axis=1)
        columns = jnp.transpose(site)[:width]
        for f in range(5):
            column = columns[:, f : f + 1]
            if f >= 2:
                column = column * VIEW_SCALE
            pix_ref[f, block * width : (block + 1) * width, :] = jnp.broadcast_to(column, (width, LANES))
    frames = unit_ref[:, SLIP_ROWS:ROWS, :].astype(jnp.float32).reshape(LANES, LANES)
    turned = jnp.transpose(frames)
    total = acc_ref[...]
    step = 16
    for group in range(GROUPS):
        base = FRAME_STRIDE * group
        rows = (turned[base : base + 8] + turned[base + 8 : base + 16]) + turned[base + 16 : base + 24]
        def spread(i):
            return jnp.broadcast_to(rows[i : i + 1], (step, LANES))
        src_e, src_n, d, s, c, sd, cd = [spread(i) for i in range(7)]
        dd = d * d
        d_sd = d * sd
        d_cd = d * cd
        k0 = sd * (-1.0 / 6.0)
        k1 = sd * cd * (1.0 / 6.0)
        k2 = sd * sd * (1.0 / 6.0)

        def chunk(i, carry):
            start = pl.multiple_of(i * step, step)
            here = pl.ds(start, step)
            e = pix_ref[0, here, :] - src_e
            n = pix_ref[1, here, :] - src_n
            v0 = pix_ref[2, here, :]
            v1 = pix_ref[3, here, :]
            w = pix_ref[4, here, :]
            x = e * s + n * c
            y = n * s - e * c
            a = v0 * s + v1 * c
            b = v1 * s - v0 * c
            xx = x * x
            r2 = xx + y * y + dd
            rho = lax.rsqrt(r2)
            t = r2 * rho + d
            tau = 1.0 / t
            rho2 = rho * rho
            rho3 = rho2 * rho
            g = rho * tau
            g2 = g + rho2
            ga = g * tau
            gc = g * g2
            gb = ga * (g + g2)
            ax = a * x
            by = b * y
            ay = a * y
            bx = b * x
            h = ax + by
            xy = x * y
            j0 = ga * (ay + bx) - xy * (gb * h + w * gc)
            j1 = (ax * rho3 - ga * (ax - by)) + xy * (gb * (ay - bx)) + w * (g - xx * gc)
            q = y * sd - d_cd
            p = y * cd + d_sd
            f = (q * (rho3 * rho2)) * (h + w * d)
            green_ref[here, 0:LANES] = (k0 * j0 - x * f).astype(jnp.bfloat16)
            green_ref[here, LANES : 2 * LANES] = (k1 * j1 - p * f).astype(jnp.bfloat16)
            green_ref[here, 2 * LANES : 3 * LANES] = (q * f - k2 * j1).astype(jnp.bfloat16)
            return carry

        lax.fori_loop(0, pixels // step, chunk, 0, unroll=2)
        slip = [
            unit_ref[:, (k * GROUPS + group) * SUB : (k * GROUPS + group + 1) * SUB, :].reshape(LANES, LANES)
            for k in range(3)
        ]
        table = jnp.concatenate(slip, axis=0)
        total = total + jnp.dot(green_ref[...], table, preferred_element_type=jnp.float32)
    out_ref[...] = total


def unit_product(sites, unit, acc):
    pixels = sites.shape[0] * sites.shape[2]
    vmem = pl.BlockSpec(memory_space=pltpu.VMEM)
    pairs = pixels * LANES * GROUPS
    return pl.pallas_call(
        unit_kernel,
        out_shape=jax.ShapeDtypeStruct((pixels, LANES), jnp.float32),
        in_specs=[vmem, vmem, vmem],
        out_specs=vmem,
        scratch_shapes=[
            pltpu.VMEM((5, pixels, LANES), jnp.float32),
            pltpu.VMEM((pixels, 3 * LANES), jnp.bfloat16),
        ],
        cost_estimate=pl.CostEstimate(flops=pairs * 3 * LANES * 2 + pairs * 80, transcendentals=2 * pairs, bytes_accessed=2**19),
        name="unit_product",
    )(sites, unit, acc)


def residual_kernel(sites_ref, pred_ref, res_ref, sum_ref):
    blocks, _, width = sites_ref.shape
    sums = []
    for block in range(blocks):
        site = jnp.concatenate([sites_ref[block], jnp.zeros((SUB, LANES - width), jnp.float32)], axis=1)
        columns = jnp.transpose(site)[:width]
        value = pred_ref[block]
        observed = jnp.broadcast_to(columns[:, 5:6], value.shape)
        noise = jnp.broadcast_to(columns[:, 6:7], value.shape)
        mask = jnp.broadcast_to(columns[:, 7:8], value.shape)
        res = mask * (value - observed) / noise
        if block == 0:
            res_ref[...] = res
        sums.append(jnp.sum(res * res, axis=0, keepdims=True))
    sum_ref[...] = (sums[0] + sums[1]) + (sums[2] + sums[3])


def residual_part(sites, pred):
    vmem = pl.BlockSpec(memory_space=pltpu.VMEM)
    return pl.pallas_call(
        residual_kernel,
        out_shape=(
            jax.ShapeDtypeStruct(pred.shape[1:], jnp.float32),
            jax.ShapeDtypeStruct((1, LANES), jnp.float32),
        ),
        in_specs=[vmem, vmem],
        out_specs=(vmem, vmem),
        name="residual_part",
    )(sites, pred)


def per_device(
    pixel_pos,
    pixel_view,
    observed,
    noise_scale,
    valid_mask,
    patch_pos,
    patch_depth,
    segment_ids,
    seg_strike,
    seg_dip,
    slip_models,
):
    own_pixels = pixel_pos.shape[1]
    y_near, y_far = xor_pairs(4, 1), mirror_pairs(4)
    x_near, x_far = xor_pairs(4, 1), mirror_pairs(4)
    z_steps = [xor_pairs(8, 1), xor_pairs(8, 2), mirror_pairs(8)]
    core = lax.axis_index("pix").astype(jnp.int32)[None]
    piece = pack(core, seg_strike, seg_dip, patch_pos, patch_depth, segment_ids, slip_models)
    sites = jnp.concatenate(
        [pixel_pos, pixel_view, observed[None], noise_scale[None], valid_mask.astype(jnp.float32)[None]], axis=0
    )[None]

    def join(value, axis, pairs):
        return jnp.concatenate([value, lax.ppermute(value, axis, pairs)], axis=0)

    sites = join(join(sites, "y", y_near), "y", y_far)
    pieces = piece[None]
    for pairs in z_steps:
        pieces = join(pieces, "z", pairs)
    swap = xor_pairs(2, 1)
    near = join(pieces, "x", x_near)
    far = lax.ppermute(near, "x", x_far)
    near_other = lax.ppermute(near, "pix", swap)
    acc = jnp.zeros((4 * own_pixels, LANES), jnp.float32)
    acc = unit_product(sites, near, acc)
    acc = unit_product(sites, near_other, acc)
    far_other = lax.ppermute(far, "pix", swap)
    acc = unit_product(sites, far, acc)
    acc = unit_product(sites, far_other, acc)

    part = acc.reshape(4, own_pixels, LANES)
    half = own_pixels // 2

    def add(mine, axis, pairs, order):
        other = lax.ppermute(mine, axis, pairs)
        return jnp.stack([mine[i] + other[j] for i, j in enumerate(order)])

    low, high = part[:, :half], part[:, half:]
    low = add(low, "y", y_near, (1, 0, 3, 2))
    high = add(high, "y", y_far, (2, 3, 0, 1))
    low = add(low, "y", y_far, (2, 3, 0, 1))
    high = add(high, "y", y_near, (1, 0, 3, 2))
    pred = jnp.concatenate([low, high], axis=1)
    residual, own_sum = residual_part(sites, pred)
    total = own_sum
    for axis, pairs in [("pix", swap), ("x", x_near), ("x", xor_pairs(4, 2))] + [("z", pairs) for pairs in z_steps]:
        total = total + lax.ppermute(total, axis, pairs)
    pixels = own_pixels * lax.axis_size(PATCH) * lax.axis_size("pix")
    return (residual, total[0] / pixels)


def solution(mesh):
    finer = Mesh(mesh.devices.reshape(4, 8, 4, mesh.shape["pix"]), PATCH_PIX)
    placed = (
        P(None, PATCH_PIX),
        P(None, PATCH_PIX),
        P(PATCH_PIX),
        P(PATCH_PIX),
        P(PATCH_PIX),
        P(None, PATCH),
        P(PATCH),
        P(PATCH),
        P(),
        P(),
        P(PATCH, None, None),
    )
    return jax.shard_map(
        per_device,
        mesh=finer,
        in_specs=placed,
        out_specs=(P(PATCH_PIX, None), P()),
        check_vma=False,
    )
```

```python
import functools
import math

import jax
import jax.numpy as jnp
from jax import lax
from jax.experimental import pallas as pl
from jax.experimental.pallas import tpu as pltpu
from jax.sharding import Mesh
from jax.sharding import PartitionSpec as P

PATCH = ("y", "z", "x")
PATCH_PIX = ("y", "z", "x", "pix")

LANES = 128
SUB = 8
GROUPS = 3
PIECE = SUB * GROUPS
SLIP_ROWS = 3 * PIECE
ROWS = SLIP_ROWS + SUB
FRAME_STRIDE = 40
NEAR_ORDER = (1, 0, 3, 2)
FAR_ORDER = (2, 3, 0, 1)
VIEW_SCALE = 3.0 / (2.0 * math.pi)


def xor_pairs(count, mask):
    return [(i, i ^ mask) for i in range(count)]


def mirror_pairs(count):
    return [(i, count - 1 - i) for i in range(count)]


VMEM_SPEC = pl.BlockSpec(memory_space=pltpu.VMEM)


LIMITS = pltpu.CompilerParams(vmem_limit_bytes=12 * 2**20)


def vmem_array(shape, dtype):
    return pltpu.VMEM(shape, dtype)


def in_vmem(array):
    return pltpu.with_memory_space_constraint(array, pltpu.VMEM)


def rounded(value):
    return value.astype(jnp.bfloat16).astype(jnp.float32)


def pack_kernel(core_ref, strike_ref, dip_ref, pos_ref, depth_ref, ids_ref, slip_ref, out_ref, turned_ref):
    ids = ids_ref[...]
    strike = jnp.zeros(ids.shape, jnp.float32)
    dip = jnp.zeros(ids.shape, jnp.float32)
    for segment in range(strike_ref.shape[0]):
        same = ids == segment
        strike = jnp.where(same, strike_ref[segment], strike)
        dip = jnp.where(same, dip_ref[segment], dip)
    pos = pos_ref[...]
    angles = jnp.concatenate([strike, dip], axis=0)
    sines = jnp.sin(angles)
    cosines = jnp.cos(angles)
    rows = jnp.concatenate(
        [pos, depth_ref[...], sines[0:1], cosines[0:1], sines[1:2], cosines[1:2], jnp.zeros(ids.shape, jnp.float32)],
        axis=0,
    )
    high = rounded(rows)
    rest = rows - high
    middle = rounded(rest)
    low = rounded(rest - middle)
    count = rows.shape[1]
    pieces = jnp.concatenate([high, middle, low], axis=0)
    pieces = jnp.concatenate([pieces, jnp.zeros((24, LANES - count), jnp.float32)], axis=1)
    pieces = jnp.concatenate([pieces, jnp.zeros((LANES - 24, LANES), jnp.float32)], axis=0)
    turned_ref[...] = jnp.transpose(pieces)
    first = core_ref[0] * PIECE
    tile = jnp.zeros((SUB, LANES), jnp.float32)
    for group in range(GROUPS):
        start = pl.multiple_of(first + SUB * group, SUB)
        part = turned_ref[pl.ds(start, SUB), :]
        tile = tile + (part if group == 0 else pltpu.roll(part, FRAME_STRIDE * group, 1))
        for k in range(3):
            row = (k * GROUPS + group) * SUB
            out_ref[row : row + SUB, :] = slip_ref[k, pl.ds(start, SUB), :]
    out_ref[SLIP_ROWS:ROWS, :] = tile.astype(jnp.bfloat16)


def pack(core, seg_strike, seg_dip, patch_pos, patch_depth, segment_ids, slip):
    smem = pl.BlockSpec(memory_space=pltpu.SMEM)
    vmem = pl.BlockSpec(memory_space=pltpu.VMEM)
    return pl.pallas_call(
        pack_kernel,
        out_shape=vmem_array((ROWS, LANES), jnp.bfloat16),
        in_specs=[smem, smem, smem, vmem, vmem, vmem, vmem],
        out_specs=vmem,
        scratch_shapes=[pltpu.VMEM((LANES, LANES), jnp.float32)],
        compiler_params=LIMITS,
        name="pack",
    )(core, seg_strike, seg_dip, patch_pos, patch_depth[None, :], segment_ids[None, :], jnp.transpose(slip, (1, 0, 2)))


def columns_kernel(sites_ref, pix_ref):
    blocks, _, width = sites_ref.shape
    for block in range(blocks):
        site = jnp.concatenate([sites_ref[block], jnp.zeros((SUB, LANES - width), jnp.float32)], axis=1)
        columns = jnp.transpose(site)[:width]
        for f in range(SUB):
            column = columns[:, f : f + 1]
            if 2 <= f < 5:
                column = column * VIEW_SCALE
            pix_ref[f, block * width : (block + 1) * width, :] = jnp.broadcast_to(column, (width, LANES))


def pixel_columns(sites):
    pixels = sites.shape[0] * sites.shape[2]
    return pl.pallas_call(
        columns_kernel,
        out_shape=vmem_array((SUB, pixels, LANES), jnp.float32),
        in_specs=[VMEM_SPEC],
        out_specs=VMEM_SPEC,
        compiler_params=LIMITS,
        name="pixel_columns",
    )(in_vmem(sites))


def unit_kernel(has_acc, pix_ref, unit_ref, *refs):
    acc_ref = refs[0] if has_acc else None
    out_ref, green_ref = refs[-2:]
    pixels = pix_ref.shape[1]
    frames = unit_ref[:, SLIP_ROWS:ROWS, :].astype(jnp.float32).reshape(LANES, LANES)
    turned = jnp.transpose(frames)
    step = 16
    span = 64

    def table_of(group):
        slip = [
            unit_ref[:, (k * GROUPS + group) * SUB : (k * GROUPS + group + 1) * SUB, :].reshape(LANES, LANES)
            for k in range(3)
        ]
        return jnp.concatenate(slip, axis=0)

    def add_product(group, here):
        value = jnp.dot(green_ref[group % 2, here, :], table_of(group), preferred_element_type=jnp.float32)
        if group == 0:
            if has_acc:
                value = value + acc_ref[here, :]
        else:
            value = value + out_ref[here, :]
        out_ref[here, :] = value

    for group in range(GROUPS):
        base = FRAME_STRIDE * group
        rows = (turned[base : base + 8] + turned[base + 8 : base + 16]) + turned[base + 16 : base + 24]

        def spread(i):
            return jnp.broadcast_to(rows[i : i + 1], (step, LANES))

        src_e, src_n, d, s, c, sd, cd = [spread(i) for i in range(7)]
        dd = d * d
        d_sd = d * sd
        d_cd = d * cd
        k0 = sd * (-1.0 / 6.0)
        k1 = sd * cd * (1.0 / 6.0)
        k2 = sd * sd * (1.0 / 6.0)

        def chunk(start):
            here = pl.ds(start, step)
            e = pix_ref[0, here, :] - src_e
            n = pix_ref[1, here, :] - src_n
            v0 = pix_ref[2, here, :]
            v1 = pix_ref[3, here, :]
            w = pix_ref[4, here, :]
            x = e * s + n * c
            y = n * s - e * c
            a = v0 * s + v1 * c
            b = v1 * s - v0 * c
            xx = x * x
            r2 = xx + y * y + dd
            rho = lax.rsqrt(r2)
            t = r2 * rho + d
            tau = 1.0 / t
            rho2 = rho * rho
            rho3 = rho2 * rho
            g = rho * tau
            g2 = g + rho2
            ga = g * tau
            gc = g * g2
            gb = ga * (g + g2)
            ax = a * x
            by = b * y
            ay = a * y
            bx = b * x
            h = ax + by
            xy = x * y
            j0 = ga * (ay + bx) - xy * (gb * h + w * gc)
            j1 = (ax * rho3 - ga * (ax - by)) + xy * (gb * (ay - bx)) + w * (g - xx * gc)
            q = y * sd - d_cd
            p = y * cd + d_sd
            f = (q * (rho3 * rho2)) * (h + w * d)
            slot = group % 2
            green_ref[slot, here, 0:LANES] = (k0 * j0 - x * f).astype(jnp.bfloat16)
            green_ref[slot, here, LANES : 2 * LANES] = (k1 * j1 - p * f).astype(jnp.bfloat16)
            green_ref[slot, here, 2 * LANES : 3 * LANES] = (q * f - k2 * j1).astype(jnp.bfloat16)

        def stretch(i, carry):
            start = pl.multiple_of(i * span, span)
            if group > 0:
                add_product(group - 1, pl.ds(start, span))
            for j in range(span // step):
                chunk(pl.multiple_of(start + j * step, step))
            return carry

        lax.fori_loop(0, pixels // span, stretch, 0)
    add_product(GROUPS - 1, pl.ds(0, pixels))


def unit_product(pix, unit, acc=None):
    pixels = pix.shape[1]
    pairs = pixels * LANES * GROUPS
    arrays = [pix, unit] if acc is None else [pix, unit, acc]
    return pl.pallas_call(
        functools.partial(unit_kernel, acc is not None),
        out_shape=vmem_array((pixels, LANES), jnp.float32),
        in_specs=[VMEM_SPEC] * len(arrays),
        out_specs=VMEM_SPEC,
        scratch_shapes=[pltpu.VMEM((2, pixels, 3 * LANES), jnp.bfloat16)],
        cost_estimate=pl.CostEstimate(flops=pairs * 1000, transcendentals=2 * pairs, bytes_accessed=2**19),
        compiler_params=LIMITS,
        name="unit_product",
    )(*[in_vmem(array) for array in arrays])


def residual_kernel(pix_ref, low_ref, low_got_ref, high_ref, high_got_ref, res_ref, sum_ref):
    half = low_ref.shape[1]
    sums = []
    for block in range(4):
        total = jnp.zeros((1, LANES), jnp.float32)
        for part, (mine, got, order) in enumerate(
            [(low_ref, low_got_ref, FAR_ORDER), (high_ref, high_got_ref, NEAR_ORDER)]
        ):
            value = mine[block] + got[order[block]]
            here = slice(block * 2 * half + part * half, block * 2 * half + (part + 1) * half)
            res = pix_ref[7, here, :] * (value - pix_ref[5, here, :]) / pix_ref[6, here, :]
            if block == 0:
                res_ref[part * half : (part + 1) * half, :] = res
            total = total + jnp.sum(res * res, axis=0, keepdims=True)
        sums.append(total)
    sum_ref[...] = (sums[0] + sums[1]) + (sums[2] + sums[3])


def residual_part(pix, low, low_got, high, high_got):
    return pl.pallas_call(
        residual_kernel,
        out_shape=(
            jax.ShapeDtypeStruct((2 * low.shape[1], LANES), jnp.float32),
            vmem_array((1, LANES), jnp.float32),
        ),
        in_specs=[VMEM_SPEC] * 5,
        out_specs=(VMEM_SPEC, VMEM_SPEC),
        compiler_params=LIMITS,
        name="residual_part",
    )(*[in_vmem(array) for array in (pix, low, low_got, high, high_got)])


def exchange_add_kernel(low_ref, low_got_ref, high_ref, high_got_ref, low_out_ref, high_out_ref):
    for i in range(4):
        low_out_ref[i] = low_ref[i] + low_got_ref[NEAR_ORDER[i]]
        high_out_ref[i] = high_ref[i] + high_got_ref[FAR_ORDER[i]]


def exchange_add(low, low_got, high, high_got):
    return pl.pallas_call(
        exchange_add_kernel,
        out_shape=(vmem_array(low.shape, jnp.float32), vmem_array(high.shape, jnp.float32)),
        in_specs=[VMEM_SPEC] * 4,
        out_specs=(VMEM_SPEC, VMEM_SPEC),
        compiler_params=LIMITS,
        name="exchange_add",
    )(*[in_vmem(array) for array in (low, low_got, high, high_got)])


def per_device(
    pixel_pos,
    pixel_view,
    observed,
    noise_scale,
    valid_mask,
    patch_pos,
    patch_depth,
    segment_ids,
    seg_strike,
    seg_dip,
    slip_models,
):
    own_pixels = pixel_pos.shape[1]
    y_near, y_far = xor_pairs(4, 1), mirror_pairs(4)
    x_near, x_far = xor_pairs(4, 1), mirror_pairs(4)
    z_steps = [xor_pairs(8, 1), xor_pairs(8, 2), mirror_pairs(8)]
    core = lax.axis_index("pix").astype(jnp.int32)[None]
    piece = pack(core, seg_strike, seg_dip, patch_pos, patch_depth, segment_ids, slip_models)
    sites = jnp.concatenate(
        [pixel_pos, pixel_view, observed[None], noise_scale[None], valid_mask.astype(jnp.float32)[None]], axis=0
    )[None]

    def join(value, axis, pairs):
        return jnp.concatenate([value, lax.ppermute(value, axis, pairs)], axis=0)

    pieces = piece[None]
    pieces, sites = lax.optimization_barrier((join(pieces, "z", z_steps[0]), join(sites, "y", y_near)))
    pieces, sites = lax.optimization_barrier((join(pieces, "z", z_steps[1]), join(sites, "y", y_far)))
    pix = pixel_columns(sites)
    pieces = join(pieces, "z", z_steps[2])
    swap = xor_pairs(2, 1)
    near = join(pieces, "x", x_near)
    far = lax.ppermute(near, "x", x_far)
    near_other = lax.ppermute(near, "pix", swap)
    acc = unit_product(pix, near)
    near_other, acc = lax.optimization_barrier((near_other, acc))
    acc = unit_product(pix, near_other, acc)
    far, acc = lax.optimization_barrier((far, acc))
    far_other = lax.ppermute(far, "pix", swap)
    acc = unit_product(pix, far, acc)
    far_other, acc = lax.optimization_barrier((far_other, acc))
    acc = unit_product(pix, far_other, acc)

    part = acc.reshape(4, own_pixels, LANES)
    half = own_pixels // 2
    low, high = part[:, :half], part[:, half:]
    low, high = exchange_add(low, lax.ppermute(low, "y", y_near), high, lax.ppermute(high, "y", y_far))
    residual, own_sum = residual_part(
        pix, low, lax.ppermute(low, "y", y_far), high, lax.ppermute(high, "y", y_near)
    )
    total = own_sum
    for axis, pairs in [("pix", swap), ("x", x_near), ("x", xor_pairs(4, 2))] + [("z", pairs) for pairs in z_steps]:
        total = total + lax.ppermute(total, axis, pairs)
    pixels = own_pixels * lax.axis_size(PATCH) * lax.axis_size("pix")
    return (residual, total[0] / pixels)


def solution(mesh):
    finer = Mesh(mesh.devices.reshape(4, 8, 4, mesh.shape["pix"]), PATCH_PIX)
    placed = (
        P(None, PATCH_PIX),
        P(None, PATCH_PIX),
        P(PATCH_PIX),
        P(PATCH_PIX),
        P(PATCH_PIX),
        P(None, PATCH),
        P(PATCH),
        P(PATCH),
        P(),
        P(),
        P(PATCH, None, None),
    )
    return jax.shard_map(
        per_device,
        mesh=finer,
        in_specs=placed,
        out_specs=(P(PATCH_PIX, None), P()),
        check_vma=False,
    )
```

```python
import functools
import math

import jax
import jax.numpy as jnp
from jax import lax
from jax.experimental import pallas as pl
from jax.experimental.pallas import tpu as pltpu
from jax.sharding import Mesh
from jax.sharding import PartitionSpec as P


PATCH = ("y", "z", "x")
PATCH_PIX = ("y", "z", "x", "pix")

LANES = 128
SUB = 8
GROUPS = 3
PIECE = SUB * GROUPS
SLIP_ROWS = 3 * PIECE
ROWS = SLIP_ROWS + SUB
FRAME_STRIDE = 40
NEAR_ORDER = (1, 0, 3, 2)
FAR_ORDER = (2, 3, 0, 1)
VIEW_SCALE = 3.0 / (2.0 * math.pi)


def xor_pairs(count, mask):
    return [(i, i ^ mask) for i in range(count)]


def mirror_pairs(count):
    return [(i, count - 1 - i) for i in range(count)]


VMEM_SPEC = pl.BlockSpec(memory_space=pltpu.VMEM)


LIMITS = pltpu.CompilerParams(vmem_limit_bytes=12 * 2**20)


def vmem_array(shape, dtype):
    return pltpu.VMEM(shape, dtype)


def in_hbm(array):
    return pltpu.with_memory_space_constraint(array, pltpu.HBM)


def in_vmem(array):
    return pltpu.with_memory_space_constraint(array, pltpu.VMEM)


def rounded(value):
    return value.astype(jnp.bfloat16).astype(jnp.float32)


def prepare_kernel(
    core_ref,
    strike_ref,
    dip_ref,
    pos_ref,
    depth_ref,
    ids_ref,
    slip_ref,
    pixel_ref,
    view_ref,
    observed_ref,
    noise_ref,
    mask_ref,
    out_ref,
    sites_ref,
    turned_ref,
):
    ids = ids_ref[...]
    strike = jnp.zeros(ids.shape, jnp.float32)
    dip = jnp.zeros(ids.shape, jnp.float32)
    for segment in range(strike_ref.shape[0]):
        same = ids == segment
        strike = jnp.where(same, strike_ref[segment], strike)
        dip = jnp.where(same, dip_ref[segment], dip)
    pos = pos_ref[...]
    angles = jnp.concatenate([strike, dip], axis=0)
    sines = jnp.sin(angles)
    cosines = jnp.cos(angles)
    rows = jnp.concatenate(
        [pos, depth_ref[...], sines[0:1], cosines[0:1], sines[1:2], cosines[1:2], jnp.zeros(ids.shape, jnp.float32)],
        axis=0,
    )
    high = rounded(rows)
    rest = rows - high
    middle = rounded(rest)
    low = rounded(rest - middle)
    count = rows.shape[1]
    pieces = jnp.concatenate([high, middle, low], axis=0)
    pieces = jnp.concatenate([pieces, jnp.zeros((24, LANES - count), jnp.float32)], axis=1)
    pieces = jnp.concatenate([pieces, jnp.zeros((LANES - 24, LANES), jnp.float32)], axis=0)
    turned_ref[...] = jnp.transpose(pieces)
    first = core_ref[0] * PIECE
    tile = jnp.zeros((SUB, LANES), jnp.float32)
    for group in range(GROUPS):
        start = pl.multiple_of(first + SUB * group, SUB)
        part = turned_ref[pl.ds(start, SUB), :]
        tile = tile + (part if group == 0 else pltpu.roll(part, FRAME_STRIDE * group, 1))
        for k in range(3):
            row = (k * GROUPS + group) * SUB
            out_ref[row : row + SUB, :] = slip_ref[k, pl.ds(start, SUB), :]
    out_ref[SLIP_ROWS:ROWS, :] = tile.astype(jnp.bfloat16)
    site = jnp.concatenate(
        [pixel_ref[...], view_ref[...], observed_ref[...], noise_ref[...], mask_ref[...].astype(jnp.float32)], axis=0
    )
    sites_ref[0] = jnp.concatenate([site, jnp.zeros((SUB, LANES - site.shape[1]), jnp.float32)], axis=1)


def prepare(core, tables, patches, pixels):
    smem = pl.BlockSpec(memory_space=pltpu.SMEM)
    vectors = list(patches) + list(pixels)
    return pl.pallas_call(
        prepare_kernel,
        out_shape=(vmem_array((ROWS, LANES), jnp.bfloat16), vmem_array((1, SUB, LANES), jnp.float32)),
        in_specs=[smem] * 3 + [VMEM_SPEC] * len(vectors),
        out_specs=(VMEM_SPEC, VMEM_SPEC),
        scratch_shapes=[pltpu.VMEM((LANES, LANES), jnp.float32)],
        compiler_params=LIMITS,
        name="prepare",
    )(core, *[in_hbm(array) for array in list(tables) + vectors])


def columns_kernel(width, sites_ref, pix_ref):
    blocks = sites_ref.shape[0]
    half = width // 2
    for block in range(blocks):
        columns = jnp.transpose(sites_ref[block])[:width]
        for f in range(SUB):
            column = columns[:, f : f + 1]
            if 2 <= f < 5:
                column = column * VIEW_SCALE
            column = jnp.broadcast_to(column, (width, LANES))
            for part in range(2):
                row = (part * blocks + block) * half
                pix_ref[f, row : row + half, :] = column[part * half : (part + 1) * half]


def pixel_columns(sites, width):
    return pl.pallas_call(
        functools.partial(columns_kernel, width),
        out_shape=vmem_array((SUB, sites.shape[0] * width, LANES), jnp.float32),
        in_specs=[VMEM_SPEC],
        out_specs=VMEM_SPEC,
        compiler_params=LIMITS,
        name="pixel_columns",
    )(in_vmem(sites))


def unit_kernel(units, count, has_acc, first_row, pix_ref, *refs):
    parts_refs = refs[:count]
    acc_ref = refs[count] if has_acc else None
    out_ref, green_ref = refs[-2:]
    pixels = out_ref.shape[0]
    step = 16
    span = 96 if pixels % 96 == 0 else pixels

    def gathered(unit, row, rows):
        return jnp.concatenate(
            [parts_refs[which][start : start + size, row : row + rows, :] for which, start, size in units[unit]], axis=0
        )

    def table_of(index):
        unit, group = divmod(index, GROUPS)
        slip = [gathered(unit, (k * GROUPS + group) * SUB, SUB).reshape(LANES, LANES) for k in range(3)]
        return jnp.concatenate(slip, axis=0)

    def add_product(index, start, size):
        here = pl.ds(start, size)
        value = jnp.dot(green_ref[index % 2, here, :], table_of(index), preferred_element_type=jnp.float32)
        if index > 0:
            value = value + out_ref[here, :]
        elif has_acc:
            value = value + acc_ref[pl.ds(first_row + start, size), :]
        out_ref[here, :] = value

    for index in range(GROUPS * len(units)):
        unit, group = divmod(index, GROUPS)
        if group == 0:
            turned = jnp.transpose(gathered(unit, SLIP_ROWS, SUB).astype(jnp.float32).reshape(LANES, LANES))
        base = FRAME_STRIDE * group
        rows = (turned[base : base + 8] + turned[base + 8 : base + 16]) + turned[base + 16 : base + 24]

        def spread(i):
            return jnp.broadcast_to(rows[i : i + 1], (step, LANES))

        src_e, src_n, d, s, c, sd, cd = [spread(i) for i in range(7)]
        dd = d * d
        d_sd = d * sd
        d_cd = d * cd
        k0 = sd * (-1.0 / 6.0)
        k1 = sd * cd * (1.0 / 6.0)
        k2 = sd * sd * (1.0 / 6.0)

        def chunk(start):
            here = pl.ds(start, step)
            src = pl.ds(first_row + start, step)
            e = pix_ref[0, src, :] - src_e
            n = pix_ref[1, src, :] - src_n
            v0 = pix_ref[2, src, :]
            v1 = pix_ref[3, src, :]
            w = pix_ref[4, src, :]
            x = e * s + n * c
            y = n * s - e * c
            a = v0 * s + v1 * c
            b = v1 * s - v0 * c
            xx = x * x
            r2 = xx + y * y + dd
            rho = lax.rsqrt(r2)
            t = r2 * rho + d
            tau = 1.0 / t
            rho2 = rho * rho
            rho3 = rho2 * rho
            g = rho * tau
            g2 = g + rho2
            ga = g * tau
            gc = g * g2
            gb = ga * (g + g2)
            ax = a * x
            by = b * y
            ay = a * y
            bx = b * x
            h = ax + by
            xy = x * y
            j0 = ga * (ay + bx) - xy * (gb * h + w * gc)
            j1 = (ax * rho3 - ga * (ax - by)) + xy * (gb * (ay - bx)) + w * (g - xx * gc)
            q = y * sd - d_cd
            p = y * cd + d_sd
            f = (q * (rho3 * rho2)) * (h + w * d)
            slot = index % 2
            green_ref[slot, here, 0:LANES] = (k0 * j0 - x * f).astype(jnp.bfloat16)
            green_ref[slot, here, LANES : 2 * LANES] = (k1 * j1 - p * f).astype(jnp.bfloat16)
            green_ref[slot, here, 2 * LANES : 3 * LANES] = (q * f - k2 * j1).astype(jnp.bfloat16)

        def stretch(i, carry):
            start = pl.multiple_of(i * span, span)
            if index > 0:
                add_product(index - 1, start, span)
            for j in range(span // step):
                chunk(pl.multiple_of(start + j * step, step))
            return carry

        lax.fori_loop(0, pixels // span, stretch, 0)
    add_product(GROUPS * len(units) - 1, 0, pixels)


def unit_product(pix, parts, units, acc=None, first_row=0, pixels=None):
    pixels = pixels or pix.shape[1]
    pairs = pixels * LANES * GROUPS * len(units)
    arrays = [pix, *parts] + ([] if acc is None else [acc])
    return pl.pallas_call(
        functools.partial(unit_kernel, units, len(parts), acc is not None, first_row),
        out_shape=vmem_array((pixels, LANES), jnp.float32),
        in_specs=[VMEM_SPEC] * len(arrays),
        out_specs=VMEM_SPEC,
        scratch_shapes=[pltpu.VMEM((2, pixels, 3 * LANES), jnp.bfloat16)],
        compiler_params=LIMITS,
        cost_estimate=pl.CostEstimate(flops=pairs * 1000, transcendentals=2 * pairs, bytes_accessed=2**19),
        name="unit_product",
    )(*[in_vmem(array) for array in arrays])


def residual_kernel(pix_ref, low_ref, low_got_ref, high_ref, high_got_ref, res_ref, sum_ref):
    half = low_ref.shape[1]
    sums = []
    for block in range(4):
        total = jnp.zeros((1, LANES), jnp.float32)
        for part, (mine, got, order) in enumerate(
            [(low_ref, low_got_ref, NEAR_ORDER), (high_ref, high_got_ref, FAR_ORDER)]
        ):
            value = mine[block] + got[order[block]]
            row = (part * 4 + block) * half
            here = slice(row, row + half)
            res = pix_ref[7, here, :] * (value - pix_ref[5, here, :]) / pix_ref[6, here, :]
            if block == 0:
                res_ref[part * half : (part + 1) * half, :] = res
            total = total + jnp.sum(res * res, axis=0, keepdims=True)
        sums.append(total)
    sum_ref[...] = (sums[0] + sums[1]) + (sums[2] + sums[3])


def residual_part(pix, low, low_got, high, high_got):
    return pl.pallas_call(
        residual_kernel,
        out_shape=(
            jax.ShapeDtypeStruct((2 * low.shape[1], LANES), jnp.float32),
            vmem_array((1, LANES), jnp.float32),
        ),
        in_specs=[VMEM_SPEC] * 5,
        out_specs=(VMEM_SPEC, VMEM_SPEC),
        compiler_params=LIMITS,
        name="residual_part",
    )(*[in_vmem(array) for array in (pix, low, low_got, high, high_got)])


def exchange_add_kernel(order, mine_ref, got_ref, out_ref):
    for i in range(4):
        out_ref[i] = mine_ref[i] + got_ref[order[i]]


def exchange_add(mine, got, order):
    return pl.pallas_call(
        functools.partial(exchange_add_kernel, order),
        out_shape=vmem_array(mine.shape, jnp.float32),
        in_specs=[VMEM_SPEC] * 2,
        out_specs=VMEM_SPEC,
        compiler_params=LIMITS,
        name="exchange_add",
    )(in_vmem(mine), in_vmem(got))


def quad_sum(value, axis, core):
    count = lax.axis_size(axis)
    low = [(2 * (i ^ 1), 2 * i) for i in range(count)]
    high = [(2 * (i ^ 2) + 1, 2 * i + 1) for i in range(count)]
    first = lax.ppermute(value, (axis, "pix"), low + high)
    second = lax.ppermute(value, (axis, "pix"), [(2 * (i ^ 3) + 1, 2 * i + 1) for i in range(count)])
    half = first + jnp.where(core == 0, value, second)
    return half + lax.ppermute(half, "pix", xor_pairs(2, 1))


def per_device(
    pixel_pos,
    pixel_view,
    observed,
    noise_scale,
    valid_mask,
    patch_pos,
    patch_depth,
    segment_ids,
    seg_strike,
    seg_dip,
    slip_models,
):
    own_pixels = pixel_pos.shape[1]
    near_pairs, far_pairs, swap = xor_pairs(4, 1), xor_pairs(4, 3), xor_pairs(2, 1)
    core = lax.axis_index("pix").astype(jnp.int32)
    piece, sites = prepare(
        core[None],
        (seg_strike, seg_dip),
        (patch_pos, patch_depth[None], segment_ids[None], jnp.transpose(slip_models, (1, 0, 2))),
        (pixel_pos, pixel_view, observed[None], noise_scale[None], valid_mask[None]),
    )

    def stack(*values):
        return jnp.concatenate(values, axis=0)

    piece = piece[None]
    two, sites = lax.optimization_barrier(
        (stack(piece, lax.ppermute(piece, "z", xor_pairs(8, 2))), stack(sites, lax.ppermute(sites, "y", near_pairs)))
    )
    sites_far = lax.ppermute(sites, "y", far_pairs)
    four = stack(two, lax.ppermute(two, "z", mirror_pairs(8)))
    four_got = lax.ppermute(four, "z", xor_pairs(8, 1))
    far_a = lax.ppermute(four, "x", far_pairs)
    near_a = lax.ppermute(four, "x", near_pairs)
    pix = pixel_columns(stack(sites, sites_far), own_pixels)
    far_b = lax.ppermute(four_got, "x", far_pairs)
    near_b = lax.ppermute(four_got, "x", near_pairs)
    own_other = lax.ppermute(stack(four, four_got), "pix", swap)
    across_a = lax.ppermute(far_a, "x", near_pairs)
    part = four.shape[0]
    count = 2 * part
    acc = unit_product(pix, (four, four_got, own_other), (((0, 0, part), (1, 0, part), (2, 0, count)),))
    near_a, near_b, far_b, acc = lax.optimization_barrier((near_a, near_b, far_b, acc))
    across_b = lax.ppermute(far_b, "x", near_pairs)
    others = lax.ppermute(stack(near_a, near_b, far_a, far_b), "pix", swap)
    acc = unit_product(
        pix,
        (near_a, near_b, far_a, far_b, others),
        (((0, 0, part), (1, 0, part), (4, 0, count)), ((2, 0, part), (3, 0, part), (4, count, count))),
        acc,
    )
    across_a, across_b, acc = lax.optimization_barrier((across_a, across_b, acc))
    across = stack(across_a, across_b)
    across_other = lax.ppermute(across, "pix", swap)
    last = (((0, 0, count), (1, 0, count)),)
    rows = 2 * own_pixels
    shape = (4, own_pixels // 2, LANES)
    low = unit_product(pix, (across, across_other), last, acc, 0, rows).reshape(shape)
    high = unit_product(pix, (across, across_other), last, acc, rows, rows).reshape(shape)
    low = exchange_add(low, lax.ppermute(low, "y", far_pairs), FAR_ORDER)
    high = exchange_add(high, lax.ppermute(high, "y", near_pairs), NEAR_ORDER)
    residual, own_sum = residual_part(
        pix, low, lax.ppermute(low, "y", near_pairs), high, lax.ppermute(high, "y", far_pairs)
    )
    total = own_sum + lax.ppermute(own_sum, "pix", swap)
    total = quad_sum(total, "x", core)
    total = quad_sum(total, "z", core)
    total = total + lax.ppermute(total, "z", mirror_pairs(8))
    pixels = own_pixels * lax.axis_size(PATCH) * lax.axis_size("pix")
    return (residual, total[0] / pixels)


def solution(mesh):
    finer = Mesh(mesh.devices.reshape(4, 8, 4, mesh.shape["pix"]), PATCH_PIX)
    placed = (
        P(None, PATCH_PIX),
        P(None, PATCH_PIX),
        P(PATCH_PIX),
        P(PATCH_PIX),
        P(PATCH_PIX),
        P(None, PATCH),
        P(PATCH),
        P(PATCH),
        P(),
        P(),
        P(PATCH, None, None),
    )
    return jax.shard_map(
        per_device,
        mesh=finer,
        in_specs=placed,
        out_specs=(P(PATCH_PIX, None), P()),
        check_vma=False,
    )
```

```python
import functools
import math

import jax
import jax.numpy as jnp
from jax import lax
from jax.experimental import pallas as pl
from jax.experimental.pallas import tpu as pltpu
from jax.sharding import Mesh
from jax.sharding import PartitionSpec as P


PATCH = ("y", "z", "x")
PATCH_PIX = ("y", "z", "x", "pix")

LANES = 128
SUB = 8
GROUPS = 3
PIECE = SUB * GROUPS
SLIP_ROWS = 3 * PIECE
ROWS = SLIP_ROWS + SUB
FRAME_STRIDE = 40
NEAR_ORDER = (1, 0, 3, 2)
FAR_ORDER = (2, 3, 0, 1)
VIEW_SCALE = 3.0 / (2.0 * math.pi)


def xor_pairs(count, mask):
    return [(i, i ^ mask) for i in range(count)]


def mirror_pairs(count):
    return [(i, count - 1 - i) for i in range(count)]


VMEM_SPEC = pl.BlockSpec(memory_space=pltpu.VMEM)


LIMITS = pltpu.CompilerParams(vmem_limit_bytes=12 * 2**20)


def vmem_array(shape, dtype):
    return pltpu.VMEM(shape, dtype)


def in_hbm(array):
    return pltpu.with_memory_space_constraint(array, pltpu.HBM)


def in_vmem(array):
    return pltpu.with_memory_space_constraint(array, pltpu.VMEM)


def rounded(value):
    return value.astype(jnp.bfloat16).astype(jnp.float32)


def prepare_kernel(
    strike_ref,
    dip_ref,
    pos_ref,
    depth_ref,
    ids_ref,
    slip_ref,
    pixel_ref,
    view_ref,
    observed_ref,
    noise_ref,
    mask_ref,
    out_ref,
    sites_ref,
    turned_ref,
):
    ids = ids_ref[...]
    strike = jnp.zeros(ids.shape, jnp.float32)
    dip = jnp.zeros(ids.shape, jnp.float32)
    for segment in range(strike_ref.shape[0]):
        same = ids == segment
        strike = jnp.where(same, strike_ref[segment], strike)
        dip = jnp.where(same, dip_ref[segment], dip)
    pos = pos_ref[...]
    angles = jnp.concatenate([strike, dip], axis=0)
    sines = jnp.sin(angles)
    cosines = jnp.cos(angles)
    rows = jnp.concatenate(
        [pos, depth_ref[...], sines[0:1], cosines[0:1], sines[1:2], cosines[1:2], jnp.zeros(ids.shape, jnp.float32)],
        axis=0,
    )
    high = rounded(rows)
    rest = rows - high
    middle = rounded(rest)
    low = rounded(rest - middle)
    count = rows.shape[1]
    pieces = jnp.concatenate([high, middle, low], axis=0)
    pieces = jnp.concatenate([pieces, jnp.zeros((24, LANES - count), jnp.float32)], axis=1)
    pieces = jnp.concatenate([pieces, jnp.zeros((LANES - 24, LANES), jnp.float32)], axis=0)
    turned_ref[...] = jnp.transpose(pieces)
    for half in range(2):
        tile = jnp.zeros((SUB, LANES), jnp.float32)
        for group in range(GROUPS):
            start = half * PIECE + SUB * group
            part = turned_ref[start : start + SUB, :]
            tile = tile + (part if group == 0 else pltpu.roll(part, FRAME_STRIDE * group, 1))
            for k in range(3):
                row = (k * GROUPS + group) * SUB
                out_ref[half, row : row + SUB, :] = slip_ref[k, start : start + SUB, :]
        out_ref[half, SLIP_ROWS:ROWS, :] = tile.astype(jnp.bfloat16)
    site = jnp.concatenate(
        [pixel_ref[...], view_ref[...], observed_ref[...], noise_ref[...], mask_ref[...].astype(jnp.float32)], axis=0
    )
    sites_ref[0] = jnp.concatenate([site, jnp.zeros((SUB, LANES - site.shape[1]), jnp.float32)], axis=1)


def prepare(tables, patches, pixels):
    smem = pl.BlockSpec(memory_space=pltpu.SMEM)
    vectors = list(patches) + list(pixels)
    return pl.pallas_call(
        prepare_kernel,
        out_shape=(vmem_array((2, ROWS, LANES), jnp.bfloat16), vmem_array((1, SUB, LANES), jnp.float32)),
        in_specs=[smem] * 2 + [VMEM_SPEC] * len(vectors),
        out_specs=(VMEM_SPEC, VMEM_SPEC),
        scratch_shapes=[pltpu.VMEM((LANES, LANES), jnp.float32)],
        compiler_params=LIMITS,
        name="prepare",
    )(*[in_hbm(array) for array in list(tables) + vectors])


def columns_kernel(width, first, sites_ref, *refs):
    pix_ref = refs[-1]
    half = width // 2
    for block in range(sites_ref.shape[0]):
        columns = jnp.transpose(sites_ref[block])[:width]
        for f in range(7):
            column = columns[:, f : f + 1]
            if 2 <= f < 5:
                column = column * VIEW_SCALE
            if f == 6:
                column = columns[:, 7:8] / column
            column = jnp.broadcast_to(column, (width, LANES))
            for part in range(2):
                row = (part * 4 + first + block) * half
                pix_ref[f, row : row + half, :] = column[part * half : (part + 1) * half]


def pixel_columns(sites, width, first, before=None):
    arrays = [sites] if before is None else [sites, before]
    return pl.pallas_call(
        functools.partial(columns_kernel, width, first),
        out_shape=vmem_array((7, 4 * width, LANES), jnp.float32),
        in_specs=[VMEM_SPEC] * len(arrays),
        out_specs=VMEM_SPEC,
        input_output_aliases={} if before is None else {1: 0},
        compiler_params=LIMITS,
        name="pixel_columns",
    )(*[in_vmem(array) for array in arrays])


def unit_kernel(units, count, has_acc, first_row, pix_ref, *refs):
    parts_refs = refs[:count]
    acc_ref = refs[count] if has_acc else None
    out_ref, green_ref = refs[-2:]
    pixels = out_ref.shape[0]
    step = 16
    span = 192

    def gathered(unit, row, rows):
        return jnp.concatenate(
            [parts_refs[which][start : start + size, row : row + rows, :] for which, start, size in units[unit]], axis=0
        )

    def table_of(index):
        unit, group = divmod(index, GROUPS)
        slip = [gathered(unit, (k * GROUPS + group) * SUB, SUB).reshape(LANES, LANES) for k in range(3)]
        return jnp.concatenate(slip, axis=0)

    def add_product(index, start, size):
        here = pl.ds(start, size)
        value = jnp.dot(green_ref[index % 2, here, :], table_of(index), preferred_element_type=jnp.float32)
        if index > 0:
            value = value + out_ref[here, :]
        elif has_acc:
            value = value + acc_ref[pl.ds(first_row + start, size), :]
        out_ref[here, :] = value

    for index in range(GROUPS * len(units)):
        unit, group = divmod(index, GROUPS)
        if group == 0:
            turned = jnp.transpose(gathered(unit, SLIP_ROWS, SUB).astype(jnp.float32).reshape(LANES, LANES))
        base = FRAME_STRIDE * group
        rows = (turned[base : base + 8] + turned[base + 8 : base + 16]) + turned[base + 16 : base + 24]

        def spread(i):
            return jnp.broadcast_to(rows[i : i + 1], (step, LANES))

        src_e, src_n, d, s, c, sd, cd = [spread(i) for i in range(7)]
        dd = d * d
        d_sd = d * sd
        d_cd = d * cd
        k0 = sd * (-1.0 / 6.0)
        k1 = sd * cd * (1.0 / 6.0)
        k2 = sd * sd * (1.0 / 6.0)

        def chunk(start):
            here = pl.ds(start, step)
            src = pl.ds(first_row + start, step)
            e = pix_ref[0, src, :] - src_e
            n = pix_ref[1, src, :] - src_n
            v0 = pix_ref[2, src, :]
            v1 = pix_ref[3, src, :]
            w = pix_ref[4, src, :]
            x = e * s + n * c
            y = n * s - e * c
            a = v0 * s + v1 * c
            b = v1 * s - v0 * c
            xx = x * x
            r2 = xx + y * y + dd
            rho = lax.rsqrt(r2)
            t = r2 * rho + d
            tau = 1.0 / t
            rho2 = rho * rho
            rho3 = rho2 * rho
            g = rho * tau
            g2 = g + rho2
            ga = g * tau
            gc = g * g2
            gb = ga * (g + g2)
            ax = a * x
            by = b * y
            ay = a * y
            bx = b * x
            h = ax + by
            xy = x * y
            j0 = ga * (ay + bx) - xy * (gb * h + w * gc)
            j1 = (ax * rho3 - ga * (ax - by)) + xy * (gb * (ay - bx)) + w * (g - xx * gc)
            q = y * sd - d_cd
            p = y * cd + d_sd
            f = (q * (rho3 * rho2)) * (h + w * d)
            slot = index % 2
            green_ref[slot, here, 0:LANES] = (k0 * j0 - x * f).astype(jnp.bfloat16)
            green_ref[slot, here, LANES : 2 * LANES] = (k1 * j1 - p * f).astype(jnp.bfloat16)
            green_ref[slot, here, 2 * LANES : 3 * LANES] = (q * f - k2 * j1).astype(jnp.bfloat16)

        def stretch(i, carry):
            start = pl.multiple_of(i * span, span)
            if index > 0:
                add_product(index - 1, start, span)
            for j in range(span // step):
                chunk(pl.multiple_of(start + j * step, step))
            return carry

        lax.fori_loop(0, pixels // span, stretch, 0)
    add_product(GROUPS * len(units) - 1, 0, pixels)


def unit_product(pix, parts, units, acc=None, first_row=0, pixels=None):
    pixels = pixels or pix.shape[1]
    pairs = pixels * LANES * GROUPS * len(units)
    arrays = [pix, *parts] + ([] if acc is None else [acc])
    return pl.pallas_call(
        functools.partial(unit_kernel, units, len(parts), acc is not None, first_row),
        out_shape=vmem_array((pixels, LANES), jnp.float32),
        in_specs=[VMEM_SPEC] * len(arrays),
        out_specs=VMEM_SPEC,
        scratch_shapes=[pltpu.VMEM((2, pixels, 3 * LANES), jnp.bfloat16)],
        compiler_params=LIMITS,
        cost_estimate=pl.CostEstimate(flops=pairs * 1000, transcendentals=2 * pairs, bytes_accessed=2**19),
        name="unit_product",
    )(*[in_vmem(array) for array in arrays])


def residual_kernel(pix_ref, low_ref, low_got_ref, high_ref, high_got_ref, res_ref, sum_ref):
    half = low_ref.shape[1]
    sums = []
    for block in range(4):
        total = jnp.zeros((1, LANES), jnp.float32)
        for part, (mine, got, order) in enumerate(
            [(low_ref, low_got_ref, NEAR_ORDER), (high_ref, high_got_ref, FAR_ORDER)]
        ):
            value = mine[block] + got[order[block]]
            row = (part * 4 + block) * half
            here = slice(row, row + half)
            res = (value - pix_ref[5, here, :]) * pix_ref[6, here, :]
            if block == 0:
                res_ref[part * half : (part + 1) * half, :] = res
            total = total + jnp.sum(res * res, axis=0, keepdims=True)
        sums.append(total)
    sum_ref[...] = (sums[0] + sums[1]) + (sums[2] + sums[3])


def residual_part(pix, low, low_got, high, high_got):
    return pl.pallas_call(
        residual_kernel,
        out_shape=(
            jax.ShapeDtypeStruct((2 * low.shape[1], LANES), jnp.float32),
            vmem_array((1, LANES), jnp.float32),
        ),
        in_specs=[VMEM_SPEC] * 5,
        out_specs=(VMEM_SPEC, VMEM_SPEC),
        compiler_params=LIMITS,
        name="residual_part",
    )(*[in_vmem(array) for array in (pix, low, low_got, high, high_got)])


def exchange_add_kernel(order, mine_ref, got_ref, out_ref):
    for i in range(4):
        out_ref[i] = mine_ref[i] + got_ref[order[i]]


def exchange_add(mine, got, order):
    return pl.pallas_call(
        functools.partial(exchange_add_kernel, order),
        out_shape=vmem_array(mine.shape, jnp.float32),
        in_specs=[VMEM_SPEC] * 2,
        out_specs=VMEM_SPEC,
        compiler_params=LIMITS,
        name="exchange_add",
    )(in_vmem(mine), in_vmem(got))


def per_device(
    pixel_pos,
    pixel_view,
    observed,
    noise_scale,
    valid_mask,
    patch_pos,
    patch_depth,
    segment_ids,
    seg_strike,
    seg_dip,
    slip_models,
):
    own_pixels = pixel_pos.shape[1]
    near_pairs, far_pairs, swap = xor_pairs(4, 1), xor_pairs(4, 3), xor_pairs(2, 1)
    core = lax.axis_index("pix").astype(jnp.int32)
    piece, sites = prepare(
        (seg_strike, seg_dip),
        (patch_pos, patch_depth[None], segment_ids[None], jnp.transpose(slip_models, (1, 0, 2))),
        (pixel_pos, pixel_view, observed[None], noise_scale[None], valid_mask[None]),
    )

    def stack(*values):
        return jnp.concatenate(values, axis=0)

    meets = [(2 * (i ^ 2), 2 * i) for i in range(8)] + [(2 * (i ^ 5) + 1, 2 * i + 1) for i in range(8)]
    first = lax.ppermute(piece, ("z", "pix"), meets)
    meets = [(2 * (i ^ 1), 2 * i) for i in range(8)] + [(2 * (i ^ 6) + 1, 2 * i + 1) for i in range(8)]
    second = lax.ppermute(piece, ("z", "pix"), meets)
    sites_near = lax.ppermute(sites, "y", near_pairs)
    four = jnp.where(core == 0, stack(piece, first), stack(first, second))
    four, sites = lax.optimization_barrier((four, stack(sites, sites_near)))
    four_got = lax.ppermute(four, "z", xor_pairs(8, 1))
    far_a = lax.ppermute(four, "x", far_pairs)
    near_a = lax.ppermute(four, "x", near_pairs)
    sites_far = lax.ppermute(sites, "y", far_pairs)
    pix = pixel_columns(sites, own_pixels, 0)
    pix = pixel_columns(sites_far, own_pixels, 2, pix)
    far_b = lax.ppermute(four_got, "x", far_pairs)
    near_b = lax.ppermute(four_got, "x", near_pairs)
    own_other = lax.ppermute(stack(four, four_got), "pix", swap)
    across_a = lax.ppermute(far_a, "x", near_pairs)
    part = four.shape[0]
    count = 2 * part
    acc = unit_product(pix, (four, four_got, own_other), (((0, 0, part), (1, 0, part), (2, 0, count)),))
    near_a, near_b, far_b, acc = lax.optimization_barrier((near_a, near_b, far_b, acc))
    across_b = lax.ppermute(far_b, "x", near_pairs)
    others = lax.ppermute(stack(near_a, near_b, far_a, far_b), "pix", swap)
    acc = unit_product(
        pix, (near_a, near_b, others), (((0, 0, part), (1, 0, part), (2, 0, count)),), acc
    )
    across_a, across_b, acc = lax.optimization_barrier((across_a, across_b, acc))
    across = stack(across_a, across_b)
    across_other = lax.ppermute(across, "pix", swap)
    acc = unit_product(
        pix, (far_a, far_b, others), (((0, 0, part), (1, 0, part), (2, count, count)),), acc
    )
    across_other, acc = lax.optimization_barrier((across_other, acc))
    last = (((0, 0, count), (1, 0, count)),)
    rows = 2 * own_pixels
    shape = (4, own_pixels // 2, LANES)
    low = unit_product(pix, (across, across_other), last, acc, 0, rows).reshape(shape)
    high = unit_product(pix, (across, across_other), last, acc, rows, rows).reshape(shape)
    low = exchange_add(low, lax.ppermute(low, "y", far_pairs), FAR_ORDER)
    high = exchange_add(high, lax.ppermute(high, "y", near_pairs), NEAR_ORDER)
    residual, own_sum = residual_part(
        pix, low, lax.ppermute(low, "y", near_pairs), high, lax.ppermute(high, "y", far_pairs)
    )
    total = own_sum + lax.ppermute(own_sum, "pix", swap)
    for axis, pairs in [
        ("x", near_pairs),
        ("x", far_pairs),
        ("z", xor_pairs(8, 1)),
        ("z", xor_pairs(8, 2)),
        ("z", mirror_pairs(8)),
    ]:
        meets = [(2 * source + 1, 2 * target + 1) for source, target in pairs]
        meets += [(2 * i, 2 * (i ^ 1)) for i, _ in pairs]
        total = total + lax.ppermute(total, (axis, "pix"), meets)
    total = jnp.where(core == 1, total, lax.ppermute(total, "pix", swap))
    pixels = own_pixels * lax.axis_size(PATCH) * lax.axis_size("pix")
    return (residual, total[0] / pixels)


def solution(mesh):
    finer = Mesh(mesh.devices.reshape(4, 8, 4, mesh.shape["pix"]), PATCH_PIX)
    placed = (
        P(None, PATCH_PIX),
        P(None, PATCH_PIX),
        P(PATCH_PIX),
        P(PATCH_PIX),
        P(PATCH_PIX),
        P(None, PATCH),
        P(PATCH),
        P(PATCH),
        P(),
        P(),
        P(PATCH, None, None),
    )
    return jax.shard_map(
        per_device,
        mesh=finer,
        in_specs=placed,
        out_specs=(P(PATCH_PIX, None), P()),
        check_vma=False,
    )
```

```python
import functools
import math

import jax
import jax.numpy as jnp
from jax import lax
from jax.experimental import pallas as pl
from jax.experimental.pallas import tpu as pltpu
from jax.sharding import Mesh
from jax.sharding import PartitionSpec as P


PATCH = ("y", "z", "x")
PATCH_PIX = ("y", "z", "x", "pix")

LANES = 128
SUB = 8
GROUPS = 3
PIECE = SUB * GROUPS
SLIP_ROWS = 3 * PIECE
ROWS = SLIP_ROWS + SUB
FRAME_STRIDE = 40
NEAR_ORDER = (1, 0, 3, 2)
FAR_ORDER = (2, 3, 0, 1)
FIRST_SHARE = 7


def shares(width):
    first = width * FIRST_SHARE // 12
    return ((0, first, 0), (first, width - first, 4 * first))


VIEW_SCALE = 3.0 / (2.0 * math.pi)


def xor_pairs(count, mask):
    return [(i, i ^ mask) for i in range(count)]


def mirror_pairs(count):
    return [(i, count - 1 - i) for i in range(count)]


VMEM_SPEC = pl.BlockSpec(memory_space=pltpu.VMEM)


LIMITS = pltpu.CompilerParams(vmem_limit_bytes=12 * 2**20)


def vmem_array(shape, dtype):
    return pltpu.VMEM(shape, dtype)


def in_hbm(array):
    return pltpu.with_memory_space_constraint(array, pltpu.HBM)


def in_vmem(array):
    return pltpu.with_memory_space_constraint(array, pltpu.VMEM)


def rounded(value):
    return value.astype(jnp.bfloat16).astype(jnp.float32)


def prepare_kernel(
    strike_ref,
    dip_ref,
    pos_ref,
    depth_ref,
    ids_ref,
    slip_ref,
    pixel_ref,
    view_ref,
    observed_ref,
    noise_ref,
    mask_ref,
    out_ref,
    sites_ref,
    turned_ref,
):
    ids = ids_ref[...]
    strike = jnp.zeros(ids.shape, jnp.float32)
    dip = jnp.zeros(ids.shape, jnp.float32)
    for segment in range(strike_ref.shape[0]):
        same = ids == segment
        strike = jnp.where(same, strike_ref[segment], strike)
        dip = jnp.where(same, dip_ref[segment], dip)
    pos = pos_ref[...]
    angles = jnp.concatenate([strike, dip], axis=0)
    sines = jnp.sin(angles)
    cosines = jnp.cos(angles)
    rows = jnp.concatenate(
        [pos, depth_ref[...], sines[0:1], cosines[0:1], sines[1:2], cosines[1:2], jnp.zeros(ids.shape, jnp.float32)],
        axis=0,
    )
    high = rounded(rows)
    rest = rows - high
    middle = rounded(rest)
    low = rounded(rest - middle)
    count = rows.shape[1]
    pieces = jnp.concatenate([high, middle, low], axis=0)
    pieces = jnp.concatenate([pieces, jnp.zeros((24, LANES - count), jnp.float32)], axis=1)
    pieces = jnp.concatenate([pieces, jnp.zeros((LANES - 24, LANES), jnp.float32)], axis=0)
    turned_ref[...] = jnp.transpose(pieces)
    for half in range(2):
        tile = jnp.zeros((SUB, LANES), jnp.float32)
        for group in range(GROUPS):
            start = half * PIECE + SUB * group
            part = turned_ref[start : start + SUB, :]
            tile = tile + (part if group == 0 else pltpu.roll(part, FRAME_STRIDE * group, 1))
            for k in range(3):
                row = (k * GROUPS + group) * SUB
                out_ref[half, row : row + SUB, :] = slip_ref[k, start : start + SUB, :]
        out_ref[half, SLIP_ROWS:ROWS, :] = tile.astype(jnp.bfloat16)
    site = jnp.concatenate(
        [pixel_ref[...], view_ref[...], observed_ref[...], noise_ref[...], mask_ref[...].astype(jnp.float32)], axis=0
    )
    sites_ref[0] = jnp.concatenate([site, jnp.zeros((SUB, LANES - site.shape[1]), jnp.float32)], axis=1)


def prepare(tables, patches, pixels):
    smem = pl.BlockSpec(memory_space=pltpu.SMEM)
    vectors = list(patches) + list(pixels)
    return pl.pallas_call(
        prepare_kernel,
        out_shape=(vmem_array((2, ROWS, LANES), jnp.bfloat16), vmem_array((1, SUB, LANES), jnp.float32)),
        in_specs=[smem] * 2 + [VMEM_SPEC] * len(vectors),
        out_specs=(VMEM_SPEC, VMEM_SPEC),
        scratch_shapes=[pltpu.VMEM((LANES, LANES), jnp.float32)],
        compiler_params=LIMITS,
        name="prepare",
    )(*[in_hbm(array) for array in list(tables) + vectors])


def columns_kernel(width, first, sites_ref, *refs):
    pix_ref = refs[-1]
    for block in range(sites_ref.shape[0]):
        columns = jnp.transpose(sites_ref[block])[:width]
        for f in range(7):
            column = columns[:, f : f + 1]
            if 2 <= f < 5:
                column = column * VIEW_SCALE
            if f == 6:
                column = columns[:, 7:8] / column
            column = jnp.broadcast_to(column, (width, LANES))
            for start, size, offset in shares(width):
                row = offset + (first + block) * size
                pix_ref[f, row : row + size, :] = column[start : start + size]


def pixel_columns(sites, width, first, before=None):
    arrays = [sites] if before is None else [sites, before]
    return pl.pallas_call(
        functools.partial(columns_kernel, width, first),
        out_shape=vmem_array((7, 4 * width, LANES), jnp.float32),
        in_specs=[VMEM_SPEC] * len(arrays),
        out_specs=VMEM_SPEC,
        input_output_aliases={} if before is None else {1: 0},
        compiler_params=LIMITS,
        name="pixel_columns",
    )(*[in_vmem(array) for array in arrays])


def unit_kernel(units, count, has_acc, first_row, pix_ref, *refs):
    parts_refs = refs[:count]
    acc_ref = refs[count] if has_acc else None
    out_ref, green_ref = refs[-2:]
    pixels = out_ref.shape[0]
    step = 16
    span = pixels // 2

    def gathered(unit, row, rows):
        return jnp.concatenate(
            [parts_refs[which][start : start + size, row : row + rows, :] for which, start, size in units[unit]], axis=0
        )

    def table_of(index):
        unit, group = divmod(index, GROUPS)
        slip = [gathered(unit, (k * GROUPS + group) * SUB, SUB).reshape(LANES, LANES) for k in range(3)]
        return jnp.concatenate(slip, axis=0)

    def add_product(index, start, size):
        here = pl.ds(start, size)
        value = jnp.dot(green_ref[index % 2, here, :], table_of(index), preferred_element_type=jnp.float32)
        if index > 0:
            value = value + out_ref[here, :]
        elif has_acc:
            value = value + acc_ref[pl.ds(first_row + start, size), :]
        out_ref[here, :] = value

    for index in range(GROUPS * len(units)):
        unit, group = divmod(index, GROUPS)
        if group == 0:
            turned = jnp.transpose(gathered(unit, SLIP_ROWS, SUB).astype(jnp.float32).reshape(LANES, LANES))
        base = FRAME_STRIDE * group
        rows = (turned[base : base + 8] + turned[base + 8 : base + 16]) + turned[base + 16 : base + 24]

        def spread(i):
            return jnp.broadcast_to(rows[i : i + 1], (step, LANES))

        src_e, src_n, d, s, c, sd, cd = [spread(i) for i in range(7)]
        dd = d * d
        d_sd = d * sd
        d_cd = d * cd
        k0 = sd * (-1.0 / 6.0)
        k1 = sd * cd * (1.0 / 6.0)
        k2 = sd * sd * (1.0 / 6.0)

        def chunk(start):
            here = pl.ds(start, step)
            src = pl.ds(first_row + start, step)
            e = pix_ref[0, src, :] - src_e
            n = pix_ref[1, src, :] - src_n
            v0 = pix_ref[2, src, :]
            v1 = pix_ref[3, src, :]
            w = pix_ref[4, src, :]
            x = e * s + n * c
            y = n * s - e * c
            a = v0 * s + v1 * c
            b = v1 * s - v0 * c
            xx = x * x
            r2 = xx + y * y + dd
            rho = lax.rsqrt(r2)
            t = r2 * rho + d
            tau = 1.0 / t
            rho2 = rho * rho
            rho3 = rho2 * rho
            g = rho * tau
            g2 = g + rho2
            ga = g * tau
            gc = g * g2
            gb = ga * (g + g2)
            ax = a * x
            by = b * y
            ay = a * y
            bx = b * x
            h = ax + by
            xy = x * y
            j0 = ga * (ay + bx) - xy * (gb * h + w * gc)
            j1 = (ax * rho3 - ga * (ax - by)) + xy * (gb * (ay - bx)) + w * (g - xx * gc)
            q = y * sd - d_cd
            p = y * cd + d_sd
            f = (q * (rho3 * rho2)) * (h + w * d)
            slot = index % 2
            green_ref[slot, here, 0:LANES] = (k0 * j0 - x * f).astype(jnp.bfloat16)
            green_ref[slot, here, LANES : 2 * LANES] = (k1 * j1 - p * f).astype(jnp.bfloat16)
            green_ref[slot, here, 2 * LANES : 3 * LANES] = (q * f - k2 * j1).astype(jnp.bfloat16)

        def stretch(i, carry):
            start = pl.multiple_of(i * span, span)
            if index > 0:
                add_product(index - 1, start, span)
            for j in range(span // step):
                chunk(pl.multiple_of(start + j * step, step))
            return carry

        lax.fori_loop(0, pixels // span, stretch, 0)
    add_product(GROUPS * len(units) - 1, 0, pixels)


def unit_product(pix, parts, units, acc=None, first_row=0, pixels=None):
    pixels = pixels or pix.shape[1]
    pairs = pixels * LANES * GROUPS * len(units)
    arrays = [pix, *parts] + ([] if acc is None else [acc])
    return pl.pallas_call(
        functools.partial(unit_kernel, units, len(parts), acc is not None, first_row),
        out_shape=vmem_array((pixels, LANES), jnp.float32),
        in_specs=[VMEM_SPEC] * len(arrays),
        out_specs=VMEM_SPEC,
        scratch_shapes=[pltpu.VMEM((2, pixels, 3 * LANES), jnp.bfloat16)],
        compiler_params=LIMITS,
        cost_estimate=pl.CostEstimate(flops=pairs * 1000, transcendentals=2 * pairs, bytes_accessed=2**19),
        name="unit_product",
    )(*[in_vmem(array) for array in arrays])


def residual_kernel(pix_ref, low_ref, low_got_ref, high_ref, high_got_ref, res_ref, sum_ref):
    width = low_ref.shape[1] + high_ref.shape[1]
    parts = (low_ref, low_got_ref, NEAR_ORDER), (high_ref, high_got_ref, FAR_ORDER)
    sums = []
    for block in range(4):
        total = jnp.zeros((1, LANES), jnp.float32)
        for (start, size, offset), (mine, got, order) in zip(shares(width), parts):
            value = mine[block] + got[order[block]]
            here = slice(offset + block * size, offset + (block + 1) * size)
            res = (value - pix_ref[5, here, :]) * pix_ref[6, here, :]
            if block == 0:
                res_ref[start : start + size, :] = res
            total = total + jnp.sum(res * res, axis=0, keepdims=True)
        sums.append(total)
    sum_ref[...] = (sums[0] + sums[1]) + (sums[2] + sums[3])


def residual_part(pix, low, low_got, high, high_got):
    return pl.pallas_call(
        residual_kernel,
        out_shape=(
            jax.ShapeDtypeStruct((low.shape[1] + high.shape[1], LANES), jnp.float32),
            vmem_array((1, LANES), jnp.float32),
        ),
        in_specs=[VMEM_SPEC] * 5,
        out_specs=(VMEM_SPEC, VMEM_SPEC),
        compiler_params=LIMITS,
        name="residual_part",
    )(*[in_vmem(array) for array in (pix, low, low_got, high, high_got)])


def exchange_add_kernel(order, mine_ref, got_ref, out_ref):
    for i in range(4):
        out_ref[i] = mine_ref[i] + got_ref[order[i]]


def exchange_add(mine, got, order):
    return pl.pallas_call(
        functools.partial(exchange_add_kernel, order),
        out_shape=vmem_array(mine.shape, jnp.float32),
        in_specs=[VMEM_SPEC] * 2,
        out_specs=VMEM_SPEC,
        compiler_params=LIMITS,
        name="exchange_add",
    )(in_vmem(mine), in_vmem(got))


def per_device(
    pixel_pos,
    pixel_view,
    observed,
    noise_scale,
    valid_mask,
    patch_pos,
    patch_depth,
    segment_ids,
    seg_strike,
    seg_dip,
    slip_models,
):
    own_pixels = pixel_pos.shape[1]
    near_pairs, far_pairs, swap = xor_pairs(4, 1), xor_pairs(4, 3), xor_pairs(2, 1)
    core = lax.axis_index("pix").astype(jnp.int32)
    piece, sites = prepare(
        (seg_strike, seg_dip),
        (patch_pos, patch_depth[None], segment_ids[None], jnp.transpose(slip_models, (1, 0, 2))),
        (pixel_pos, pixel_view, observed[None], noise_scale[None], valid_mask[None]),
    )

    def stack(*values):
        return jnp.concatenate(values, axis=0)

    meets = [(2 * (i ^ 2), 2 * i) for i in range(8)] + [(2 * (i ^ 5) + 1, 2 * i + 1) for i in range(8)]
    first = lax.ppermute(piece, ("z", "pix"), meets)
    meets = [(2 * (i ^ 1), 2 * i) for i in range(8)] + [(2 * (i ^ 6) + 1, 2 * i + 1) for i in range(8)]
    second = lax.ppermute(piece, ("z", "pix"), meets)
    sites_near = lax.ppermute(sites, "y", near_pairs)
    four = jnp.where(core == 0, stack(piece, first), stack(first, second))
    four, sites = lax.optimization_barrier((four, stack(sites, sites_near)))
    four_got = lax.ppermute(four, "z", xor_pairs(8, 1))
    far_a = lax.ppermute(four, "x", far_pairs)
    near_a = lax.ppermute(four, "x", near_pairs)
    sites_far = lax.ppermute(sites, "y", far_pairs)
    pix = pixel_columns(sites, own_pixels, 0)
    pix = pixel_columns(sites_far, own_pixels, 2, pix)
    far_b = lax.ppermute(four_got, "x", far_pairs)
    near_b = lax.ppermute(four_got, "x", near_pairs)
    own_other = lax.ppermute(stack(four, four_got), "pix", swap)
    across_a = lax.ppermute(far_a, "x", near_pairs)
    part = four.shape[0]
    count = 2 * part
    acc = unit_product(pix, (four, four_got, own_other), (((0, 0, part), (1, 0, part), (2, 0, count)),))
    across_b = lax.ppermute(far_b, "x", near_pairs)
    others = lax.ppermute(stack(near_a, near_b, far_a, far_b), "pix", swap)
    acc = unit_product(
        pix, (near_a, near_b, others), (((0, 0, part), (1, 0, part), (2, 0, count)),), acc
    )
    across_a, across_b, acc = lax.optimization_barrier((across_a, across_b, acc))
    across = stack(across_a, across_b)
    across_other = lax.ppermute(across, "pix", swap)
    acc = unit_product(
        pix, (far_a, far_b, others), (((0, 0, part), (1, 0, part), (2, count, count)),), acc
    )
    across_other, acc = lax.optimization_barrier((across_other, acc))
    last = (((0, 0, count), (1, 0, count)),)

    def last_product(share):
        _, size, offset = share
        value = unit_product(pix, (across, across_other), last, acc, offset, 4 * size)
        return value.reshape(4, size, LANES)

    first_share, second_share = shares(own_pixels)
    low = last_product(first_share)
    high = last_product(second_share)
    low = exchange_add(low, lax.ppermute(low, "y", far_pairs), FAR_ORDER)
    high = exchange_add(high, lax.ppermute(high, "y", near_pairs), NEAR_ORDER)
    low_got = lax.ppermute(low, "y", near_pairs)
    high_got = lax.ppermute(high, "y", far_pairs)
    residual, own_sum = residual_part(pix, low, low_got, high, high_got)
    total = own_sum + lax.ppermute(own_sum, "pix", swap)
    meets = [(2 * (i ^ 1), 2 * i) for i in range(4)] + [(2 * (i ^ 2) + 1, 2 * i + 1) for i in range(4)]
    first = lax.ppermute(total, ("x", "pix"), meets)
    meets = [(2 * (i ^ 1), 2 * i) for i in range(4)] + [(2 * (i ^ 3) + 1, 2 * i + 1) for i in range(4)]
    second = lax.ppermute(total, ("x", "pix"), meets)
    total = first + jnp.where(core == 0, total, second)
    total = total + lax.ppermute(total, "pix", swap)
    for pairs in [xor_pairs(8, 1), xor_pairs(8, 2), mirror_pairs(8)]:
        meets = [(2 * source + 1, 2 * target + 1) for source, target in pairs]
        meets += [(2 * i, 2 * (i ^ 1)) for i, _ in pairs]
        total = total + lax.ppermute(total, ("z", "pix"), meets)
    total = jnp.where(core == 1, total, lax.ppermute(total, "pix", swap))
    pixels = own_pixels * lax.axis_size(PATCH) * lax.axis_size("pix")
    return (residual, total[0] / pixels)


def solution(mesh):
    finer = Mesh(mesh.devices.reshape(4, 8, 4, mesh.shape["pix"]), PATCH_PIX)
    placed = (
        P(None, PATCH_PIX),
        P(None, PATCH_PIX),
        P(PATCH_PIX),
        P(PATCH_PIX),
        P(PATCH_PIX),
        P(None, PATCH),
        P(PATCH),
        P(PATCH),
        P(),
        P(),
        P(PATCH, None, None),
    )
    return jax.shard_map(
        per_device,
        mesh=finer,
        in_specs=placed,
        out_specs=(P(PATCH_PIX, None), P()),
        check_vma=False,
    )
```

```python
import functools
import math

import jax
import jax.numpy as jnp
from jax import lax
from jax.experimental import pallas as pl
from jax.experimental.pallas import tpu as pltpu
from jax.sharding import Mesh
from jax.sharding import PartitionSpec as P


PATCH = ("y", "z", "x")
PATCH_PIX = ("y", "z", "x", "pix")

LANES = 128
SUB = 8
GROUPS = 3
PIECE = SUB * GROUPS
SLIP_ROWS = 3 * PIECE
ROWS = SLIP_ROWS + SUB
FRAME_STRIDE = 40
NEAR_ORDER = (1, 0, 3, 2)
FAR_ORDER = (2, 3, 0, 1)
FIRST_SHARE = 8


def shares(width):
    first = width * FIRST_SHARE // 12
    return ((0, first, 0), (first, width - first, 4 * first))


VIEW_SCALE = 3.0 / (2.0 * math.pi)


def xor_pairs(count, mask):
    return [(i, i ^ mask) for i in range(count)]


def mirror_pairs(count):
    return [(i, count - 1 - i) for i in range(count)]


VMEM_SPEC = pl.BlockSpec(memory_space=pltpu.VMEM)


LIMITS = pltpu.CompilerParams(vmem_limit_bytes=12 * 2**20)


def vmem_array(shape, dtype):
    return pltpu.VMEM(shape, dtype)


def in_hbm(array):
    return pltpu.with_memory_space_constraint(array, pltpu.HBM)


def in_vmem(array):
    return pltpu.with_memory_space_constraint(array, pltpu.VMEM)


def rounded(value):
    return value.astype(jnp.bfloat16).astype(jnp.float32)


def prepare_kernel(
    strike_ref,
    dip_ref,
    pos_ref,
    depth_ref,
    ids_ref,
    slip_ref,
    pixel_ref,
    view_ref,
    observed_ref,
    noise_ref,
    mask_ref,
    out_ref,
    sites_ref,
    turned_ref,
):
    ids = ids_ref[...]
    strike = jnp.zeros(ids.shape, jnp.float32)
    dip = jnp.zeros(ids.shape, jnp.float32)
    for segment in range(strike_ref.shape[0]):
        same = ids == segment
        strike = jnp.where(same, strike_ref[segment], strike)
        dip = jnp.where(same, dip_ref[segment], dip)
    pos = pos_ref[...]
    angles = jnp.concatenate([strike, dip], axis=0)
    sines = jnp.sin(angles)
    cosines = jnp.cos(angles)
    rows = jnp.concatenate(
        [pos, depth_ref[...], sines[0:1], cosines[0:1], sines[1:2], cosines[1:2], jnp.zeros(ids.shape, jnp.float32)],
        axis=0,
    )
    high = rounded(rows)
    rest = rows - high
    middle = rounded(rest)
    low = rounded(rest - middle)
    count = rows.shape[1]
    pieces = jnp.concatenate([high, middle, low], axis=0)
    pieces = jnp.concatenate([pieces, jnp.zeros((24, LANES - count), jnp.float32)], axis=1)
    pieces = jnp.concatenate([pieces, jnp.zeros((LANES - 24, LANES), jnp.float32)], axis=0)
    turned_ref[...] = jnp.transpose(pieces)
    for half in range(2):
        tile = jnp.zeros((SUB, LANES), jnp.float32)
        for group in range(GROUPS):
            start = half * PIECE + SUB * group
            part = turned_ref[start : start + SUB, :]
            tile = tile + (part if group == 0 else pltpu.roll(part, FRAME_STRIDE * group, 1))
            for k in range(3):
                row = (k * GROUPS + group) * SUB
                out_ref[half, row : row + SUB, :] = slip_ref[k, start : start + SUB, :]
        out_ref[half, SLIP_ROWS:ROWS, :] = tile.astype(jnp.bfloat16)
    site = jnp.concatenate(
        [pixel_ref[...], view_ref[...], observed_ref[...], noise_ref[...], mask_ref[...].astype(jnp.float32)], axis=0
    )
    sites_ref[0] = jnp.concatenate([site, jnp.zeros((SUB, LANES - site.shape[1]), jnp.float32)], axis=1)


def prepare(tables, patches, pixels):
    smem = pl.BlockSpec(memory_space=pltpu.SMEM)
    vectors = list(patches) + list(pixels)
    return pl.pallas_call(
        prepare_kernel,
        out_shape=(vmem_array((2, ROWS, LANES), jnp.bfloat16), vmem_array((1, SUB, LANES), jnp.float32)),
        in_specs=[smem] * 2 + [VMEM_SPEC] * len(vectors),
        out_specs=(VMEM_SPEC, VMEM_SPEC),
        scratch_shapes=[pltpu.VMEM((LANES, LANES), jnp.float32)],
        compiler_params=LIMITS,
        name="prepare",
    )(*[in_hbm(array) for array in list(tables) + vectors])


def columns_kernel(width, first, sites_ref, *refs):
    pix_ref = refs[-1]
    for block in range(sites_ref.shape[0]):
        columns = jnp.transpose(sites_ref[block])[:width]
        for f in range(7):
            column = columns[:, f : f + 1]
            if 2 <= f < 5:
                column = column * VIEW_SCALE
            if f == 6:
                column = columns[:, 7:8] / column
            column = jnp.broadcast_to(column, (width, LANES))
            for start, size, offset in shares(width):
                row = offset + (first + block) * size
                pix_ref[f, row : row + size, :] = column[start : start + size]


def pixel_columns(sites, width, first, before=None):
    arrays = [sites] if before is None else [sites, before]
    return pl.pallas_call(
        functools.partial(columns_kernel, width, first),
        out_shape=vmem_array((7, 4 * width, LANES), jnp.float32),
        in_specs=[VMEM_SPEC] * len(arrays),
        out_specs=VMEM_SPEC,
        input_output_aliases={} if before is None else {1: 0},
        compiler_params=LIMITS,
        name="pixel_columns",
    )(*[in_vmem(array) for array in arrays])


def unit_kernel(units, count, has_acc, first_row, pix_ref, *refs):
    parts_refs = refs[:count]
    acc_ref = refs[count] if has_acc else None
    out_ref, green_ref = refs[-2:]
    pixels = out_ref.shape[0]
    step = 16
    span = pixels // 2

    def gathered(unit, row, rows):
        return jnp.concatenate(
            [parts_refs[which][start : start + size, row : row + rows, :] for which, start, size in units[unit]], axis=0
        )

    def table_of(index):
        unit, group = divmod(index, GROUPS)
        slip = [gathered(unit, (k * GROUPS + group) * SUB, SUB).reshape(LANES, LANES) for k in range(3)]
        return jnp.concatenate(slip, axis=0)

    def add_product(index, start, size):
        here = pl.ds(start, size)
        value = jnp.dot(green_ref[index % 2, here, :], table_of(index), preferred_element_type=jnp.float32)
        if index > 0:
            value = value + out_ref[here, :]
        elif has_acc:
            value = value + acc_ref[pl.ds(first_row + start, size), :]
        out_ref[here, :] = value

    for index in range(GROUPS * len(units)):
        unit, group = divmod(index, GROUPS)
        if group == 0:
            turned = jnp.transpose(gathered(unit, SLIP_ROWS, SUB).astype(jnp.float32).reshape(LANES, LANES))
        base = FRAME_STRIDE * group
        rows = (turned[base : base + 8] + turned[base + 8 : base + 16]) + turned[base + 16 : base + 24]

        def spread(i):
            return jnp.broadcast_to(rows[i : i + 1], (step, LANES))

        src_e, src_n, d, s, c, sd, cd = [spread(i) for i in range(7)]
        dd = d * d
        d_sd = d * sd
        d_cd = d * cd
        k0 = sd * (-1.0 / 6.0)
        k1 = sd * cd * (1.0 / 6.0)
        k2 = sd * sd * (1.0 / 6.0)

        def chunk(start):
            here = pl.ds(start, step)
            src = pl.ds(first_row + start, step)
            e = pix_ref[0, src, :] - src_e
            n = pix_ref[1, src, :] - src_n
            v0 = pix_ref[2, src, :]
            v1 = pix_ref[3, src, :]
            w = pix_ref[4, src, :]
            x = e * s + n * c
            y = n * s - e * c
            a = v0 * s + v1 * c
            b = v1 * s - v0 * c
            xx = x * x
            r2 = xx + y * y + dd
            rho = lax.rsqrt(r2)
            t = r2 * rho + d
            tau = 1.0 / t
            rho2 = rho * rho
            rho3 = rho2 * rho
            g = rho * tau
            g2 = g + rho2
            ga = g * tau
            gc = g * g2
            gb = ga * (g + g2)
            ax = a * x
            by = b * y
            ay = a * y
            bx = b * x
            h = ax + by
            xy = x * y
            j0 = ga * (ay + bx) - xy * (gb * h + w * gc)
            j1 = (ax * rho3 - ga * (ax - by)) + xy * (gb * (ay - bx)) + w * (g - xx * gc)
            q = y * sd - d_cd
            p = y * cd + d_sd
            f = (q * (rho3 * rho2)) * (h + w * d)
            slot = index % 2
            green_ref[slot, here, 0:LANES] = (k0 * j0 - x * f).astype(jnp.bfloat16)
            green_ref[slot, here, LANES : 2 * LANES] = (k1 * j1 - p * f).astype(jnp.bfloat16)
            green_ref[slot, here, 2 * LANES : 3 * LANES] = (q * f - k2 * j1).astype(jnp.bfloat16)

        def stretch(i, carry):
            start = pl.multiple_of(i * span, span)
            if index > 0:
                add_product(index - 1, start, span)
            for j in range(span // step):
                chunk(pl.multiple_of(start + j * step, step))
            return carry

        lax.fori_loop(0, pixels // span, stretch, 0)
    add_product(GROUPS * len(units) - 1, 0, pixels)


def unit_product(pix, parts, units, acc=None, first_row=0, pixels=None):
    pixels = pixels or pix.shape[1]
    pairs = pixels * LANES * GROUPS * len(units)
    arrays = [pix, *parts] + ([] if acc is None else [acc])
    return pl.pallas_call(
        functools.partial(unit_kernel, units, len(parts), acc is not None, first_row),
        out_shape=vmem_array((pixels, LANES), jnp.float32),
        in_specs=[VMEM_SPEC] * len(arrays),
        out_specs=VMEM_SPEC,
        scratch_shapes=[pltpu.VMEM((2, pixels, 3 * LANES), jnp.bfloat16)],
        compiler_params=LIMITS,
        cost_estimate=pl.CostEstimate(flops=pairs * 1000, transcendentals=2 * pairs, bytes_accessed=2**19),
        name="unit_product",
    )(*[in_vmem(array) for array in arrays])


def residuals(block, pix_ref, low_ref, low_got_ref, high_ref, high_got_ref):
    width = low_ref.shape[1] + high_ref.shape[1]
    parts = (low_ref, low_got_ref, NEAR_ORDER), (high_ref, high_got_ref, FAR_ORDER)
    for (start, size, offset), (mine, got, order) in zip(shares(width), parts):
        value = mine[block] + got[order[block]]
        here = slice(offset + block * size, offset + (block + 1) * size)
        yield start, size, (value - pix_ref[5, here, :]) * pix_ref[6, here, :]


def square_sum_kernel(*refs):
    sums = []
    for block in range(4):
        total = jnp.zeros((1, LANES), jnp.float32)
        for _, _, res in residuals(block, *refs[:-1]):
            total = total + jnp.sum(res * res, axis=0, keepdims=True)
        sums.append(total)
    refs[-1][...] = (sums[0] + sums[1]) + (sums[2] + sums[3])


def own_residual_kernel(*refs):
    for start, size, res in residuals(0, *refs[:-1]):
        refs[-1][start : start + size, :] = res


def on_sums(kernel, shape, arrays):
    return pl.pallas_call(
        kernel, out_shape=shape, in_specs=[VMEM_SPEC] * len(arrays), out_specs=VMEM_SPEC, compiler_params=LIMITS
    )(*[in_vmem(array) for array in arrays])


def exchange_add_kernel(order, mine_ref, got_ref, out_ref):
    for i in range(4):
        out_ref[i] = mine_ref[i] + got_ref[order[i]]


def exchange_add(mine, got, order):
    return pl.pallas_call(
        functools.partial(exchange_add_kernel, order),
        out_shape=vmem_array(mine.shape, jnp.float32),
        in_specs=[VMEM_SPEC] * 2,
        out_specs=VMEM_SPEC,
        compiler_params=LIMITS,
        name="exchange_add",
    )(in_vmem(mine), in_vmem(got))


def per_device(
    pixel_pos,
    pixel_view,
    observed,
    noise_scale,
    valid_mask,
    patch_pos,
    patch_depth,
    segment_ids,
    seg_strike,
    seg_dip,
    slip_models,
):
    own_pixels = pixel_pos.shape[1]
    near_pairs, far_pairs, swap = xor_pairs(4, 1), xor_pairs(4, 3), xor_pairs(2, 1)
    core = lax.axis_index("pix").astype(jnp.int32)
    piece, sites = prepare(
        (seg_strike, seg_dip),
        (patch_pos, patch_depth[None], segment_ids[None], jnp.transpose(slip_models, (1, 0, 2))),
        (pixel_pos, pixel_view, observed[None], noise_scale[None], valid_mask[None]),
    )

    def stack(*values):
        return jnp.concatenate(values, axis=0)

    meets = [(2 * (i ^ 2), 2 * i) for i in range(8)] + [(2 * (i ^ 5) + 1, 2 * i + 1) for i in range(8)]
    first = lax.ppermute(piece, ("z", "pix"), meets)
    meets = [(2 * (i ^ 1), 2 * i) for i in range(8)] + [(2 * (i ^ 6) + 1, 2 * i + 1) for i in range(8)]
    second = lax.ppermute(piece, ("z", "pix"), meets)
    sites_near = lax.ppermute(sites, "y", near_pairs)
    four = jnp.where(core == 0, stack(piece, first), stack(first, second))
    four, sites = lax.optimization_barrier((four, stack(sites, sites_near)))
    four_got = lax.ppermute(four, "z", xor_pairs(8, 1))
    far_a = lax.ppermute(four, "x", far_pairs)
    near_a = lax.ppermute(four, "x", near_pairs)
    sites_far = lax.ppermute(sites, "y", far_pairs)
    pix = pixel_columns(sites, own_pixels, 0)
    pix = pixel_columns(sites_far, own_pixels, 2, pix)
    far_b = lax.ppermute(four_got, "x", far_pairs)
    near_b = lax.ppermute(four_got, "x", near_pairs)
    own_other = lax.ppermute(stack(four, four_got), "pix", swap)
    across_a = lax.ppermute(far_a, "x", near_pairs)
    part = four.shape[0]
    count = 2 * part
    acc = unit_product(pix, (four, four_got, own_other), (((0, 0, part), (1, 0, part), (2, 0, count)),))
    across_b = lax.ppermute(far_b, "x", near_pairs)
    others = lax.ppermute(stack(near_a, near_b, far_a, far_b), "pix", swap)
    acc = unit_product(
        pix, (near_a, near_b, others), (((0, 0, part), (1, 0, part), (2, 0, count)),), acc
    )
    across_a, across_b, acc = lax.optimization_barrier((across_a, across_b, acc))
    across = stack(across_a, across_b)
    across_other = lax.ppermute(across, "pix", swap)
    acc = unit_product(
        pix, (far_a, far_b, others), (((0, 0, part), (1, 0, part), (2, count, count)),), acc
    )
    across_other, acc = lax.optimization_barrier((across_other, acc))
    last = (((0, 0, count), (1, 0, count)),)

    def last_product(share):
        _, size, offset = share
        value = unit_product(pix, (across, across_other), last, acc, offset, 4 * size)
        return value.reshape(4, size, LANES)

    first_share, second_share = shares(own_pixels)
    low = last_product(first_share)
    high = last_product(second_share)
    low = exchange_add(low, lax.ppermute(low, "y", far_pairs), FAR_ORDER)
    high = exchange_add(high, lax.ppermute(high, "y", near_pairs), NEAR_ORDER)
    low_got = lax.ppermute(low, "y", near_pairs)
    high_got = lax.ppermute(high, "y", far_pairs)
    sums = pix, low, low_got, high, high_got
    own_sum = on_sums(square_sum_kernel, vmem_array((1, LANES), jnp.float32), sums)
    shape = jax.ShapeDtypeStruct((own_pixels, LANES), jnp.float32)
    residual = on_sums(own_residual_kernel, shape, sums)
    total = own_sum + lax.ppermute(own_sum, "pix", swap)
    meets = [(2 * (i ^ 1), 2 * i) for i in range(4)] + [(2 * (i ^ 2) + 1, 2 * i + 1) for i in range(4)]
    first = lax.ppermute(total, ("x", "pix"), meets)
    meets = [(2 * (i ^ 1), 2 * i) for i in range(4)] + [(2 * (i ^ 3) + 1, 2 * i + 1) for i in range(4)]
    second = lax.ppermute(total, ("x", "pix"), meets)
    total = first + jnp.where(core == 0, total, second)
    total = total + lax.ppermute(total, "pix", swap)
    for pairs in [xor_pairs(8, 1), xor_pairs(8, 2), mirror_pairs(8)]:
        meets = [(2 * source + 1, 2 * target + 1) for source, target in pairs]
        meets += [(2 * i, 2 * (i ^ 1)) for i, _ in pairs]
        total = total + lax.ppermute(total, ("z", "pix"), meets)
    total = jnp.where(core == 1, total, lax.ppermute(total, "pix", swap))
    pixels = own_pixels * lax.axis_size(PATCH) * lax.axis_size("pix")
    return (residual, total[0] / pixels)


def solution(mesh):
    finer = Mesh(mesh.devices.reshape(4, 8, 4, mesh.shape["pix"]), PATCH_PIX)
    placed = (
        P(None, PATCH_PIX),
        P(None, PATCH_PIX),
        P(PATCH_PIX),
        P(PATCH_PIX),
        P(PATCH_PIX),
        P(None, PATCH),
        P(PATCH),
        P(PATCH),
        P(),
        P(),
        P(PATCH, None, None),
    )
    return jax.shard_map(
        per_device,
        mesh=finer,
        in_specs=placed,
        out_specs=(P(PATCH_PIX, None), P()),
        check_vma=False,
    )
```

```python
import functools
import math

import jax
import jax.numpy as jnp
from jax import lax
from jax.experimental import pallas as pl
from jax.experimental.pallas import tpu as pltpu
from jax.sharding import Mesh
from jax.sharding import PartitionSpec as P


PATCH = ("y", "z", "x")
PATCH_PIX = ("y", "z", "x", "pix")

LANES = 128
SUB = 8
GROUPS = 3
PIECE = SUB * GROUPS
SLIP_ROWS = 3 * PIECE
ROWS = SLIP_ROWS + SUB
FRAME_STRIDE = 40
NEAR_ORDER = (1, 0, 3, 2)
FAR_ORDER = (2, 3, 0, 1)
FIRST_SHARE = 7


def shares(width):
    first = width * FIRST_SHARE // 12
    return ((0, first, 0), (first, width - first, 4 * first))


VIEW_SCALE = 3.0 / (2.0 * math.pi)


def xor_pairs(count, mask):
    return [(i, i ^ mask) for i in range(count)]


def mirror_pairs(count):
    return [(i, count - 1 - i) for i in range(count)]


VMEM_SPEC = pl.BlockSpec(memory_space=pltpu.VMEM)


LIMITS = pltpu.CompilerParams(vmem_limit_bytes=12 * 2**20)


def vmem_array(shape, dtype):
    return pltpu.VMEM(shape, dtype)


def in_hbm(array):
    return pltpu.with_memory_space_constraint(array, pltpu.HBM)


def in_vmem(array):
    return pltpu.with_memory_space_constraint(array, pltpu.VMEM)


def rounded(value):
    return value.astype(jnp.bfloat16).astype(jnp.float32)


def prepare_kernel(
    strike_ref,
    dip_ref,
    pos_ref,
    depth_ref,
    ids_ref,
    slip_ref,
    pixel_ref,
    view_ref,
    observed_ref,
    noise_ref,
    mask_ref,
    out_ref,
    sites_ref,
    turned_ref,
):
    ids = ids_ref[...]
    strike = jnp.zeros(ids.shape, jnp.float32)
    dip = jnp.zeros(ids.shape, jnp.float32)
    for segment in range(strike_ref.shape[0]):
        same = ids == segment
        strike = jnp.where(same, strike_ref[segment], strike)
        dip = jnp.where(same, dip_ref[segment], dip)
    pos = pos_ref[...]
    angles = jnp.concatenate([strike, dip], axis=0)
    sines = jnp.sin(angles)
    cosines = jnp.cos(angles)
    rows = jnp.concatenate(
        [pos, depth_ref[...], sines[0:1], cosines[0:1], sines[1:2], cosines[1:2], jnp.zeros(ids.shape, jnp.float32)],
        axis=0,
    )
    high = rounded(rows)
    rest = rows - high
    middle = rounded(rest)
    low = rounded(rest - middle)
    count = rows.shape[1]
    pieces = jnp.concatenate([high, middle, low], axis=0)
    pieces = jnp.concatenate([pieces, jnp.zeros((24, LANES - count), jnp.float32)], axis=1)
    pieces = jnp.concatenate([pieces, jnp.zeros((LANES - 24, LANES), jnp.float32)], axis=0)
    turned_ref[...] = jnp.transpose(pieces)
    for half in range(2):
        tile = jnp.zeros((SUB, LANES), jnp.float32)
        for group in range(GROUPS):
            start = half * PIECE + SUB * group
            part = turned_ref[start : start + SUB, :]
            tile = tile + (part if group == 0 else pltpu.roll(part, FRAME_STRIDE * group, 1))
            for k in range(3):
                row = (k * GROUPS + group) * SUB
                out_ref[half, row : row + SUB, :] = slip_ref[k, start : start + SUB, :]
        out_ref[half, SLIP_ROWS:ROWS, :] = tile.astype(jnp.bfloat16)
    site = jnp.concatenate(
        [pixel_ref[...], view_ref[...], observed_ref[...], noise_ref[...], mask_ref[...].astype(jnp.float32)], axis=0
    )
    sites_ref[0] = jnp.concatenate([site, jnp.zeros((SUB, LANES - site.shape[1]), jnp.float32)], axis=1)


def prepare(tables, patches, pixels):
    smem = pl.BlockSpec(memory_space=pltpu.SMEM)
    vectors = list(patches) + list(pixels)
    return pl.pallas_call(
        prepare_kernel,
        out_shape=(vmem_array((2, ROWS, LANES), jnp.bfloat16), vmem_array((1, SUB, LANES), jnp.float32)),
        in_specs=[smem] * 2 + [VMEM_SPEC] * len(vectors),
        out_specs=(VMEM_SPEC, VMEM_SPEC),
        scratch_shapes=[pltpu.VMEM((LANES, LANES), jnp.float32)],
        compiler_params=LIMITS,
        name="prepare",
    )(*[in_hbm(array) for array in list(tables) + vectors])


def columns_kernel(width, first, sites_ref, *refs):
    pix_ref = refs[-1]
    for block in range(sites_ref.shape[0]):
        columns = jnp.transpose(sites_ref[block])[:width]
        for f in range(7):
            column = columns[:, f : f + 1]
            if 2 <= f < 5:
                column = column * VIEW_SCALE
            if f == 6:
                column = columns[:, 7:8] / column
            column = jnp.broadcast_to(column, (width, LANES))
            for start, size, offset in shares(width):
                row = offset + (first + block) * size
                pix_ref[f, row : row + size, :] = column[start : start + size]


def pixel_columns(sites, width, first, before=None):
    arrays = [sites] if before is None else [sites, before]
    return pl.pallas_call(
        functools.partial(columns_kernel, width, first),
        out_shape=vmem_array((7, 4 * width, LANES), jnp.float32),
        in_specs=[VMEM_SPEC] * len(arrays),
        out_specs=VMEM_SPEC,
        input_output_aliases={} if before is None else {1: 0},
        compiler_params=LIMITS,
        name="pixel_columns",
    )(*[in_vmem(array) for array in arrays])


def unit_kernel(units, count, has_acc, first_row, pix_ref, *refs):
    parts_refs = refs[:count]
    acc_ref = refs[count] if has_acc else None
    out_ref, green_ref = refs[-2:]
    pixels = out_ref.shape[0]
    step = 16
    span = pixels // 2

    def gathered(unit, row, rows):
        return jnp.concatenate(
            [parts_refs[which][start : start + size, row : row + rows, :] for which, start, size in units[unit]], axis=0
        )

    def table_of(index):
        unit, group = divmod(index, GROUPS)
        slip = [gathered(unit, (k * GROUPS + group) * SUB, SUB).reshape(LANES, LANES) for k in range(3)]
        return jnp.concatenate(slip, axis=0)

    def add_product(index, start, size):
        here = pl.ds(start, size)
        value = jnp.dot(green_ref[index % 2, here, :], table_of(index), preferred_element_type=jnp.float32)
        if index > 0:
            value = value + out_ref[here, :]
        elif has_acc:
            value = value + acc_ref[pl.ds(first_row + start, size), :]
        out_ref[here, :] = value

    for index in range(GROUPS * len(units)):
        unit, group = divmod(index, GROUPS)
        if group == 0:
            turned = jnp.transpose(gathered(unit, SLIP_ROWS, SUB).astype(jnp.float32).reshape(LANES, LANES))
        base = FRAME_STRIDE * group
        rows = (turned[base : base + 8] + turned[base + 8 : base + 16]) + turned[base + 16 : base + 24]

        def spread(i):
            return jnp.broadcast_to(rows[i : i + 1], (step, LANES))

        src_e, src_n, d, s, c, sd, cd = [spread(i) for i in range(7)]
        dd = d * d
        d_sd = d * sd
        d_cd = d * cd
        k0 = sd * (-1.0 / 6.0)
        k1 = sd * cd * (1.0 / 6.0)
        k2 = sd * sd * (1.0 / 6.0)

        def chunk(start):
            here = pl.ds(start, step)
            src = pl.ds(first_row + start, step)
            e = pix_ref[0, src, :] - src_e
            n = pix_ref[1, src, :] - src_n
            v0 = pix_ref[2, src, :]
            v1 = pix_ref[3, src, :]
            w = pix_ref[4, src, :]
            x = e * s + n * c
            y = n * s - e * c
            a = v0 * s + v1 * c
            b = v1 * s - v0 * c
            xx = x * x
            r2 = xx + y * y + dd
            rho = lax.rsqrt(r2)
            t = r2 * rho + d
            tau = 1.0 / t
            rho2 = rho * rho
            rho3 = rho2 * rho
            g = rho * tau
            g2 = g + rho2
            ga = g * tau
            gc = g * g2
            gb = ga * (g + g2)
            ax = a * x
            by = b * y
            ay = a * y
            bx = b * x
            h = ax + by
            xy = x * y
            j0 = ga * (ay + bx) - xy * (gb * h + w * gc)
            j1 = (ax * rho3 - ga * (ax - by)) + xy * (gb * (ay - bx)) + w * (g - xx * gc)
            q = y * sd - d_cd
            p = y * cd + d_sd
            f = (q * (rho3 * rho2)) * (h + w * d)
            slot = index % 2
            green_ref[slot, here, 0:LANES] = (k0 * j0 - x * f).astype(jnp.bfloat16)
            green_ref[slot, here, LANES : 2 * LANES] = (k1 * j1 - p * f).astype(jnp.bfloat16)
            green_ref[slot, here, 2 * LANES : 3 * LANES] = (q * f - k2 * j1).astype(jnp.bfloat16)

        def stretch(i, carry):
            start = pl.multiple_of(i * span, span)
            if index > 0:
                add_product(index - 1, start, span)
            for j in range(span // step):
                chunk(pl.multiple_of(start + j * step, step))
            return carry

        lax.fori_loop(0, pixels // span, stretch, 0)
    add_product(GROUPS * len(units) - 1, 0, pixels)


def unit_product(pix, parts, units, acc=None, first_row=0, pixels=None):
    pixels = pixels or pix.shape[1]
    pairs = pixels * LANES * GROUPS * len(units)
    arrays = [pix, *parts] + ([] if acc is None else [acc])
    return pl.pallas_call(
        functools.partial(unit_kernel, units, len(parts), acc is not None, first_row),
        out_shape=vmem_array((pixels, LANES), jnp.float32),
        in_specs=[VMEM_SPEC] * len(arrays),
        out_specs=VMEM_SPEC,
        scratch_shapes=[pltpu.VMEM((2, pixels, 3 * LANES), jnp.bfloat16)],
        compiler_params=LIMITS,
        cost_estimate=pl.CostEstimate(flops=pairs * 1000, transcendentals=2 * pairs, bytes_accessed=2**19),
        name="unit_product",
    )(*[in_vmem(array) for array in arrays])


def residuals(block, pix_ref, low_ref, low_got_ref, high_ref, high_got_ref):
    width = low_ref.shape[1] + high_ref.shape[1]
    parts = (low_ref, low_got_ref, FAR_ORDER), (high_ref, high_got_ref, NEAR_ORDER)
    for (start, size, offset), (mine, got, order) in zip(shares(width), parts):
        value = mine[block] + got[order[block]]
        here = slice(offset + block * size, offset + (block + 1) * size)
        yield start, size, (value - pix_ref[5, here, :]) * pix_ref[6, here, :]


def square_sum_kernel(*refs):
    sums = []
    for block in range(4):
        total = jnp.zeros((1, LANES), jnp.float32)
        for _, _, res in residuals(block, *refs[:-1]):
            total = total + jnp.sum(res * res, axis=0, keepdims=True)
        sums.append(total)
    refs[-1][...] = (sums[0] + sums[1]) + (sums[2] + sums[3])


def own_residual_kernel(*refs):
    for start, size, res in residuals(0, *refs[:-1]):
        refs[-1][start : start + size, :] = res


def on_sums(kernel, shape, arrays):
    return pl.pallas_call(
        kernel, out_shape=shape, in_specs=[VMEM_SPEC] * len(arrays), out_specs=VMEM_SPEC, compiler_params=LIMITS
    )(*[in_vmem(array) for array in arrays])


def exchange_add_kernel(order, mine_ref, got_ref, out_ref):
    for i in range(4):
        out_ref[i] = mine_ref[i] + got_ref[order[i]]


def exchange_add(mine, got, order):
    return pl.pallas_call(
        functools.partial(exchange_add_kernel, order),
        out_shape=vmem_array(mine.shape, jnp.float32),
        in_specs=[VMEM_SPEC] * 2,
        out_specs=VMEM_SPEC,
        compiler_params=LIMITS,
        name="exchange_add",
    )(in_vmem(mine), in_vmem(got))


def per_device(
    pixel_pos,
    pixel_view,
    observed,
    noise_scale,
    valid_mask,
    patch_pos,
    patch_depth,
    segment_ids,
    seg_strike,
    seg_dip,
    slip_models,
):
    own_pixels = pixel_pos.shape[1]
    near_pairs, far_pairs, swap = xor_pairs(4, 1), xor_pairs(4, 3), xor_pairs(2, 1)
    core = lax.axis_index("pix").astype(jnp.int32)
    piece, sites = prepare(
        (seg_strike, seg_dip),
        (patch_pos, patch_depth[None], segment_ids[None], jnp.transpose(slip_models, (1, 0, 2))),
        (pixel_pos, pixel_view, observed[None], noise_scale[None], valid_mask[None]),
    )

    def stack(*values):
        return jnp.concatenate(values, axis=0)

    meets = [(2 * (i ^ 2), 2 * i) for i in range(8)] + [(2 * (i ^ 5) + 1, 2 * i + 1) for i in range(8)]
    first = lax.ppermute(piece, ("z", "pix"), meets)
    meets = [(2 * (i ^ 1), 2 * i) for i in range(8)] + [(2 * (i ^ 6) + 1, 2 * i + 1) for i in range(8)]
    second = lax.ppermute(piece, ("z", "pix"), meets)
    sites_near = lax.ppermute(sites, "y", near_pairs)
    four = jnp.where(core == 0, stack(piece, first), stack(first, second))
    four, sites = lax.optimization_barrier((four, stack(sites, sites_near)))
    four_got = lax.ppermute(four, "z", xor_pairs(8, 1))
    far_a = lax.ppermute(four, "x", far_pairs)
    near_a = lax.ppermute(four, "x", near_pairs)
    sites_far = lax.ppermute(sites, "y", far_pairs)
    pix = pixel_columns(sites, own_pixels, 0)
    pix = pixel_columns(sites_far, own_pixels, 2, pix)
    far_b = lax.ppermute(four_got, "x", far_pairs)
    near_b = lax.ppermute(four_got, "x", near_pairs)
    own_other = lax.ppermute(stack(four, four_got), "pix", swap)
    across_a = lax.ppermute(far_a, "x", near_pairs)
    part = four.shape[0]
    count = 2 * part
    acc = unit_product(pix, (four, four_got, own_other), (((0, 0, part), (1, 0, part), (2, 0, count)),))
    across_b = lax.ppermute(far_b, "x", near_pairs)
    others = lax.ppermute(stack(near_a, near_b, far_a, far_b), "pix", swap)
    acc = unit_product(
        pix, (near_a, near_b, others), (((0, 0, part), (1, 0, part), (2, 0, count)),), acc
    )
    across_a, across_b, acc = lax.optimization_barrier((across_a, across_b, acc))
    across = stack(across_a, across_b)
    across_other = lax.ppermute(across, "pix", swap)
    acc = unit_product(
        pix, (far_a, far_b, others), (((0, 0, part), (1, 0, part), (2, count, count)),), acc
    )
    across_other, acc = lax.optimization_barrier((across_other, acc))
    last = (((0, 0, count), (1, 0, count)),)

    def last_product(share):
        _, size, offset = share
        value = unit_product(pix, (across, across_other), last, acc, offset, 4 * size)
        return value.reshape(4, size, LANES)

    first_share, second_share = shares(own_pixels)
    low = last_product(first_share)
    high = last_product(second_share)
    low = exchange_add(low, lax.ppermute(low, "y", near_pairs), NEAR_ORDER)
    high = exchange_add(high, lax.ppermute(high, "y", far_pairs), FAR_ORDER)
    low_got = lax.ppermute(low, "y", far_pairs)
    high_got = lax.ppermute(high, "y", near_pairs)
    sums = pix, low, low_got, high, high_got
    own_sum = on_sums(square_sum_kernel, vmem_array((1, LANES), jnp.float32), sums)
    shape = jax.ShapeDtypeStruct((own_pixels, LANES), jnp.float32)
    residual = on_sums(own_residual_kernel, shape, sums)
    total = own_sum + lax.ppermute(own_sum, "pix", swap)
    meets = [(2 * (i ^ 1), 2 * i) for i in range(4)] + [(2 * (i ^ 2) + 1, 2 * i + 1) for i in range(4)]
    first = lax.ppermute(total, ("x", "pix"), meets)
    meets = [(2 * (i ^ 1), 2 * i) for i in range(4)] + [(2 * (i ^ 3) + 1, 2 * i + 1) for i in range(4)]
    second = lax.ppermute(total, ("x", "pix"), meets)
    total = first + jnp.where(core == 0, total, second)
    total = total + lax.ppermute(total, "pix", swap)
    for pairs in [xor_pairs(8, 1), xor_pairs(8, 2), mirror_pairs(8)]:
        meets = [(2 * source + 1, 2 * target + 1) for source, target in pairs]
        meets += [(2 * i, 2 * (i ^ 1)) for i, _ in pairs]
        total = total + lax.ppermute(total, ("z", "pix"), meets)
    total = jnp.where(core == 1, total, lax.ppermute(total, "pix", swap))
    pixels = own_pixels * lax.axis_size(PATCH) * lax.axis_size("pix")
    return (residual, total[0] / pixels)


def solution(mesh):
    finer = Mesh(mesh.devices.reshape(4, 8, 4, mesh.shape["pix"]), PATCH_PIX)
    placed = (
        P(None, PATCH_PIX),
        P(None, PATCH_PIX),
        P(PATCH_PIX),
        P(PATCH_PIX),
        P(PATCH_PIX),
        P(None, PATCH),
        P(PATCH),
        P(PATCH),
        P(),
        P(),
        P(PATCH, None, None),
    )
    return jax.shard_map(
        per_device,
        mesh=finer,
        in_specs=placed,
        out_specs=(P(PATCH_PIX, None), P()),
        check_vma=False,
    )
```
